256 devices in a mesh: dp: 8 (over x, core), vocab: 32 (over z, y).
Axes of the slice: x: 4, y: 4, z: 8, core: 2. Of those that a mesh axis runs over, the one named last changes fastest.
Arguments:
- hidden: bfloat16 [1024, 8192], P(('dp', 'vocab')), may hold values from -350 to 350
- lm_head: bfloat16 [8192, 128256], P(None, ('dp', 'vocab')), may hold values from -0.0625 to 0.0625
- targets: int32 [1024], P(('dp', 'vocab')), may hold values from 0 to 128255
- segment: int32 [1024], P(('dp', 'vocab')), may hold values from 0 to 256, as said below
- pad_mask: int32 [1024], P(('dp', 'vocab')), may hold values from 0 to 1, as said below
- seq_bench: int32 [257], replicated, may hold values from 0 to 7
Outputs:
- token_nll: float32 [1024], P(('dp', 'vocab'))
- bench_total: float32 [8], replicated
- bench_count: float32 [8], replicated
The draws below stay inside these ranges and needn't reach their ends.
Inputs may be any that keep to these rules, and one draw needn't show every extreme that they name: `segment`: sequence numbers never fall along the pack; each aligned block of 4 tokens holds exactly one place inside it where the number rises by one, and the number does not change between one block's last token and the next block's first. `pad_mask`: the last token of each aligned block of 4 tokens is real.
All inputs are finite; a program needn't handle non-finite values.
Results may differ from the reference program's by a relative error of at most 0.0003.
Values may be sent and summed in bfloat16 or wider, within the bound.
A program may use at most 128 MiB of HBM per device.

```python
import math
import jax
import jax.numpy as jnp
import numpy as np
from jax import lax

D = 8192
VOCAB = 128256
TOK_DEV = 4
NBENCH = 8
TOKENS = 1024
NSEQ = 257


def draw_hidden(key, part):
    first, second = jax.random.split(key, 2)
    base = jnp.clip(jax.random.normal(first, (TOKENS, D), jnp.float32), -5.0, 5.0)
    scales = 3.0 * jnp.exp(jax.random.uniform(second, (TOKENS,), jnp.float32, -0.3, 0.3))
    return (base * scales[:, None]).astype(jnp.bfloat16)


def draw_segment(key, part):
    blocks = TOKENS // TOK_DEV
    places = jax.random.randint(jax.random.fold_in(key, 11), (blocks,), 1, TOK_DEV)
    local = jnp.arange(TOK_DEV, dtype=jnp.int32)
    rises = (local[None, :] >= places[:, None]).astype(jnp.int32)
    numbers = jnp.arange(blocks, dtype=jnp.int32)[:, None] + rises
    return numbers.reshape(TOKENS).astype(jnp.int32)


def draw_pad_mask(key, part):
    blocks = TOKENS // TOK_DEV
    values = jax.random.randint(jax.random.fold_in(key, 23), (blocks, TOK_DEV), 0, 4)
    real = (values != 0).astype(jnp.int32)
    last = (jnp.arange(TOK_DEV, dtype=jnp.int32) == TOK_DEV - 1).astype(jnp.int32)
    return jnp.maximum(real, last[None, :]).reshape(TOKENS).astype(jnp.int32)


def place_ends(values, rng, smallest, top_value):
    dims = values.shape
    place = [jax.random.randint(jax.random.fold_in(rng, axis), (), 0, dims[axis]) for axis in range(len(dims))]
    values = values.at[tuple(place)].set(smallest)
    longest = dims.index(max(dims))
    place[longest] = (place[longest] + 1) % dims[longest]
    return values.at[tuple(place)].set(top_value)


def block_scale(stream_key, dims, cuts, least, largest):
    def one(axis_at, parts):
        steps = jax.random.uniform(jax.random.fold_in(jax.random.fold_in(stream_key, 6), axis_at), (parts,), jnp.float32, least / len(cuts), largest / len(cuts))
        return jnp.repeat(jnp.exp(steps), dims[axis_at] // parts).reshape((-1,) + (1,) * (len(dims) - axis_at - 1))

    loudness = one(*cuts[0])
    for cut in cuts[1:]:
        loudness = loudness * one(*cut)
    return loudness


def wide_ids(rng, extent, amount, lean):
    loads = [min(1 << octave, amount + 1 - (1 << octave)) * (1 << 20) // math.isqrt((1 << octave) ** lean) + 1 for octave in range((amount + 1).bit_length()) if 1 << octave <= amount]
    width = 1 + sum(loads) // (1 << 30)
    listing = np.cumsum(np.array([max(1, weight // width) for weight in loads]))
    ticket = jax.random.randint(jax.random.fold_in(rng, 1), extent, 0, int(listing[len(loads) - 1]))
    start = jnp.left_shift(1, jnp.searchsorted(jnp.asarray(listing, jnp.int32), ticket, side="right").astype(jnp.int32))
    rank = start - 1 + jax.random.randint(jax.random.fold_in(rng, 4), extent, 0, 1 << 30) % jnp.minimum(start, amount + 1 - start)
    return jax.random.permutation(jax.random.fold_in(rng, 2), amount)[rank].astype(jnp.int32)


def scatter_about(stream_key, dims, scale, most, pieces=(), held_as=jnp.bfloat16):
    drawn = scale * jax.random.normal(stream_key, dims, jnp.float32)
    if pieces:
        drawn = drawn * block_scale(stream_key, dims, pieces, -0.22, 0.18)
    return jnp.clip(drawn, -most, most).astype(held_as)


def setup_inputs(seed: int = 0) -> dict:
    seeds = jax.random.split(jax.random.key(seed), 7)
    return {
        "hidden": draw_hidden(jax.random.fold_in(seeds[6], 71), 0),
        "lm_head": scatter_about(seeds[1], (D, VOCAB), D ** -0.5, 0.0625, ((1, 256),)),
        "targets": place_ends(wide_ids(seeds[2], (TOKENS,), VOCAB, 2), jax.random.fold_in(seeds[2], 3), 0, VOCAB - 1).astype(jnp.int32),
        "segment": draw_segment(jax.random.fold_in(seeds[6], 71), 0),
        "pad_mask": draw_pad_mask(jax.random.fold_in(seeds[6], 71), 0),
        "seq_bench": place_ends(jax.random.randint(seeds[5], (NSEQ,), 0, NBENCH), jax.random.fold_in(seeds[5], 1), 0, NBENCH - 1).astype(jnp.int32),
    }


def reference(hidden, lm_head, targets, segment, pad_mask, seq_bench):
    block = math.gcd(TOKENS, 128)

    def one_block(pair):
        rows, wanted = pair
        logits = jnp.dot(rows, lm_head, preferred_element_type=jnp.float32)
        top = jnp.max(logits, axis=1)
        total = jnp.sum(jnp.exp(logits - top[:, None]), axis=1)
        picked = jnp.take_along_axis(logits, wanted[:, None], axis=1)[:, 0]
        return top + jnp.log(total) - picked

    token_nll = lax.map(one_block, (hidden.reshape(TOKENS // block, block, D), targets.reshape(TOKENS // block, block))).reshape(TOKENS)
    following = jnp.concatenate([segment[1:], jnp.full((1,), -1, jnp.int32)])
    keep = (pad_mask * (segment == following).astype(jnp.int32)).astype(jnp.float32)
    bench = seq_bench[segment]
    bench_hot = (bench[:, None] == jnp.arange(NBENCH, dtype=jnp.int32)[None, :]).astype(jnp.float32)
    bench_total = jnp.sum(bench_hot * (keep * token_nll)[:, None], axis=0)
    bench_count = jnp.sum(bench_hot * keep[:, None], axis=0)
    return token_nll, bench_total, bench_count
```

```python
import functools

import jax
import jax.numpy as jnp
from jax import lax
from jax.experimental import pallas as pl
from jax.experimental.pallas import tpu as pltpu
from jax.sharding import Mesh
from jax.sharding import PartitionSpec as P

NBENCH = 8
AXES = ("dp_0", "dp_1", "vocab_0", "vocab_1")
NA, NB, NZ = 4, 4, 8
PIECES = 8
LAG = 6
GROUP = NA * NB * NZ
DIST = (0, NZ - 1, 1, NZ - 2, 2, NZ - 3, 3, 4)
MESH = pl.DeviceIdType.MESH
F32 = jnp.float32


def kernel(
    hidden, lm_head, targets, segment, pad_mask, seq_bench,
    nll_out, total_out, count_out,
    abuf, rows32, gath, wbuf, acc, tcol, info, stat, last, nllbuf,
    lsem, wlsem, wsend, wrecv, asend, arecv, zsend, zrecv,
    bsend, brecv, fsend, frecv, isend, irecv, ssend, srecv, csend, crecv,
):
    x, c = lax.axis_index("dp_0"), lax.axis_index("dp_1")
    z, y = lax.axis_index("vocab_0"), lax.axis_index("vocab_1")
    a = y * (1 - c) + x * c
    b = x * (1 - c) + y * c
    kp = abuf.shape[3]
    voc = lm_head.shape[1]

    def dev(a_, b_, z_, c_=None):
        if c_ is None:
            return (b_ * (1 - c) + a_ * c, c, z_, a_ * (1 - c) + b_ * c)
        return (x, c_, z, y)

    def rdma(src, dst, ssem, rsem, to):
        return pltpu.make_async_remote_copy(
            src_ref=src, dst_ref=dst, send_sem=ssem, recv_sem=rsem,
            device_id=to, device_id_type=MESH,
        )

    def a_at(k):
        return lax.rem(a + k, NA)

    def b_at(k):
        return lax.rem(b + k, NB)

    def z_at(k):
        return lax.rem(z + k, NZ)

    partner = dev(a, b, z, 1 - c)

    def own_hidden(p):
        cols = pl.ds(pl.multiple_of(p * kp, kp), kp)
        return pltpu.make_async_copy(hidden.at[:, cols], abuf.at[p, a], lsem.at[p])

    def own_weights(p):
        rows = pl.ds(pl.multiple_of(p * kp, kp), kp)
        return pltpu.make_async_copy(lm_head.at[rows, :], wbuf.at[0, rows, :], wlsem.at[p])

    def swap_weights(p):
        rows = pl.ds(pl.multiple_of(p * kp, kp), kp)
        return rdma(lm_head.at[rows, :], wbuf.at[1, rows, :], wsend, wrecv.at[p], partner)

    def loop(n, body):
        lax.fori_loop(0, n, lambda i, _: (body(i), 0)[1], 0)

    loop(PIECES, lambda p: own_hidden(p).start())

    barrier = pltpu.get_barrier_semaphore()
    peers = (
        [dev(a_at(k), b, z) for k in range(1, NA)]
        + [dev(a, b_at(k), z) for k in range(1, NB)]
        + [dev(a, b, z_at(k)) for k in range(1, NZ)]
        + [partner]
    )
    for peer in peers:
        pl.semaphore_signal(barrier, inc=1, device_id=peer, device_id_type=MESH)

    row = lax.broadcasted_iota(jnp.int32, (8, 128), 0)
    lane = lax.broadcasted_iota(jnp.int32, (8, 128), 1)
    base = z * (NA * 4) + a * 4
    own = jnp.zeros((8, 128), jnp.int32)
    whole_last = (x == NA - 1) & (c == 1) & (z == NZ - 1) & (y == NB - 1)
    for t in range(4):
        seg = segment[t]
        if t < 3:
            kept = (pad_mask[t] == 1) & (seg == segment[t + 1])
        else:
            kept = (pad_mask[t] == 1) & jnp.logical_not(whole_last)
        code = jnp.where(kept, seq_bench[seg], NBENCH)
        own = jnp.where((row == b) & (lane == base + t), targets[t], own)
        own = jnp.where((row == b + 4) & (lane == base + t), code, own)
    own = own.astype(F32)

    loop(acc.shape[1] // 64, lambda i: zero_rows(acc, i))

    pl.semaphore_wait(barrier, len(peers))

    def a_copy(p, k):
        return rdma(abuf.at[p, a], abuf.at[p, a], asend, arecv.at[p, k - 1], dev(a_at(k), b, z))

    def a_start(p):
        own_hidden(p).wait()
        for k in range(1, NA):
            a_copy(p, k).start()

    loop(PIECES, a_start)
    loop(PIECES, lambda p: own_weights(p).start())
    loop(PIECES, lambda p: swap_weights(p).start())

    def stage(buf, at, n, me, ssem, rsem, to, value):
        buf[at + me] = value
        for k in range(1, n):
            rdma(buf.at[at + me], buf.at[at + me], ssem.at[at + k], rsem.at[at + k], to(k)).start()

    def stage_wait(buf, at, n, me, ssem, rsem, to):
        for k in range(1, n):
            rdma(buf.at[at + me], buf.at[at + me], ssem.at[at + k], rsem.at[at + k], to(k)).wait()

    def to_a(k):
        return dev(a_at(k), b, z)

    def to_b(k):
        return dev(a, b_at(k), z)

    def to_z(k):
        return dev(a, b, z_at(k))

    sa, sb, sz = (0, NA, a, ), (NA, NB, b), (NA + NB, NZ, z)

    def added(buf, at, n):
        total = buf[at]
        for k in range(1, n):
            total = total + buf[at + k]
        return total

    stage(info, *sa, isend, irecv, to_a, own)

    def block(p, b_, z_):
        return gath.at[p, b_, z_]

    def z_copy(p, k, sem, up):
        zi = z_at(k)
        return rdma(block(p, b, zi), block(p, b, zi), zsend, zrecv.at[p, sem], dev(a, b, z_at(up)))

    def b_copy(p, j, way):
        zi = z_at(DIST[j])
        return rdma(
            block(p, b, zi), block(p, b, zi), bsend, brecv.at[p, way, j],
            dev(a, b_at(1 if way == 0 else NB - 1), z),
        )

    def f_copy(p, j):
        zi = z_at(DIST[j])
        come, go = (NB - 1, 1) if j % 2 == 0 else (1, NB - 1)
        return rdma(
            block(p, b_at(come), zi), block(p, b_at(come), zi), fsend, frecv.at[p, j],
            dev(a, b_at(go), z),
        )

    def b_both(p, j):
        b_copy(p, j, 0).start()
        b_copy(p, j, 1).start()

    def step_0(p):
        for k in range(1, NA):
            a_copy(p, k).wait_recv()
        for k in range(NA):
            rows32[4 * k : 4 * k + 4, :] = abuf[p, k].astype(F32)
        gath[p, b, z] = rows32[...].astype(jnp.bfloat16)
        z_copy(p, 0, 0, 1).start()
        z_copy(p, 0, 1, NZ - 1).start()
        b_both(p, 0)

    def step(p, s):
        z_copy(p, NZ - s, 2 * s - 2, 1).wait_recv()
        if s < 3:
            z_copy(p, NZ - s, 2 * s, 1).start()
        z_copy(p, s, 2 * s - 1, NZ - 1).wait_recv()
        if s < 3:
            z_copy(p, s, 2 * s + 1, NZ - 1).start()
        else:
            odd = lax.rem(p, 2)
            z_copy(p, 5 + 6 * odd, 6, 1 + 6 * odd).start()
        b_both(p, 2 * s - 1)
        b_both(p, 2 * s)

    def step_4(p):
        z_copy(p, 4, 6, 1).wait_recv()
        b_both(p, 7)

    def forward(p, s):
        for j in ((0,), (1, 2), (3, 4), (5, 6), (7,))[s]:
            b_copy(p, j, j % 2).wait_recv()
            f_copy(p, j).start()

    def multiply(p):
        for j in range(8):
            b_copy(p, j, 1 - j % 2).wait_recv()
            f_copy(p, j).wait_recv()
        own_weights(p).wait()
        swap_weights(p).wait_recv()
        rows = pl.ds(pl.multiple_of(p * kp, kp), kp)
        for w in range(2):
            lhs = gath[p].reshape(acc.shape[1], kp)
            acc[w] += jnp.dot(lhs, wbuf[w, rows, :], preferred_element_type=F32)

    def at_piece(tick, lag, fn):
        p = tick - lag

        @pl.when((p >= 0) & (p < PIECES))
        def _():
            fn(p)

    eye = lax.broadcasted_iota(jnp.int32, (128, 128), 0) == lax.broadcasted_iota(
        jnp.int32, (128, 128), 1
    )

    def ticks(tick):
        at_piece(tick, 0, step_0)
        for s in range(1, 4):
            at_piece(tick, s, functools.partial(step, s=s))
        at_piece(tick, 4, step_4)
        for s in range(5):
            at_piece(tick, s + 1, functools.partial(forward, s=s))
        at_piece(tick, LAG, multiply)

        @pl.when(tick == 2)
        def _():
            stage_wait(info, *sa, isend, irecv, to_a)
            stage(info, *sb, isend, irecv, to_b, added(info, 0, NA))

        @pl.when(tick == 4)
        def _():
            stage_wait(info, *sb, isend, irecv, to_b)
            stage(info, *sz, isend, irecv, to_z, added(info, NA, NB))

        @pl.when(tick == 6)
        def _():
            stage_wait(info, *sz, isend, irecv, to_z)
            every = added(info, NA + NB, NZ)
            info[0] = every
            for k in range(4):
                wide = jnp.where(eye, jnp.broadcast_to(every[k : k + 1, :], (128, 128)), 0.0)
                tcol[k * 128 : (k + 1) * 128, :] = jnp.sum(wide, axis=1, keepdims=True)

    loop(PIECES + LAG, ticks)

    index = ((x * 2 + c) * NZ + z) * NB + y
    other = ((x * 2 + 1 - c) * NZ + z) * NB + y
    lanes = lax.broadcasted_iota(jnp.int32, (128, voc), 1)
    cols = [(lanes + i * voc).astype(F32) for i in (index, other)]

    def statistics(k):
        rows = pl.ds(pl.multiple_of(k * 128, 128), 128)
        own_l, other_l = acc[0, rows, :], acc[1, rows, :]
        wanted = tcol[rows, :]
        top = jnp.maximum(
            jnp.max(own_l, axis=1, keepdims=True), jnp.max(other_l, axis=1, keepdims=True)
        )
        total = jnp.sum(jnp.exp(own_l - top), axis=1, keepdims=True) + jnp.sum(
            jnp.exp(other_l - top), axis=1, keepdims=True
        )
        picked = jnp.sum(
            jnp.where(cols[0] == wanted, own_l, 0.0), axis=1, keepdims=True
        ) + jnp.sum(jnp.where(cols[1] == wanted, other_l, 0.0), axis=1, keepdims=True)
        lse = top + jnp.log(total)
        for at, value in ((0, lse), (4, picked)):
            wide = jnp.where(eye, jnp.broadcast_to(value, (128, 128)), 0.0)
            nllbuf[pl.ds(at + k, 1), :] = jnp.sum(wide, axis=0, keepdims=True)

    loop(4, statistics)

    def merged(buf, at, n):
        parts = [buf[at + k] for k in range(n)]
        top = functools.reduce(jnp.maximum, parts)
        total = functools.reduce(jnp.add, [jnp.exp(part - top) for part in parts])
        picked = functools.reduce(jnp.add, parts)
        return jnp.where(row < 4, top + jnp.log(total), picked)

    stage(stat, *sa, ssend, srecv, to_a, nllbuf[...])
    stage_wait(stat, *sa, ssend, srecv, to_a)
    stage(stat, *sb, ssend, srecv, to_b, merged(stat, 0, NA))
    stage_wait(stat, *sb, ssend, srecv, to_b)
    stage(stat, *sz, ssend, srecv, to_z, merged(stat, NA, NB))
    stage_wait(stat, *sz, ssend, srecv, to_z)
    both = merged(stat, NA + NB, NZ)
    nll = both[0:4, :] - both[4:8, :]

    codes = info[0][4:8, :]
    last_t, last_c = jnp.zeros((8, 128), F32), jnp.zeros((8, 128), F32)
    for j in range(NBENCH):
        hit = codes == float(j)
        part_t = jnp.sum(jnp.where(hit, nll, 0.0), axis=0, keepdims=True)
        part_c = jnp.sum(jnp.where(hit, 1.0, 0.0), axis=0, keepdims=True)
        last_t = jnp.where(row == j, part_t, last_t)
        last_c = jnp.where(row == j, part_c, last_c)
    last[c, 0:8, :] = last_t
    last[c, 8:16, :] = last_c
    swap = rdma(last.at[c], last.at[c], csend, crecv, partner)
    swap.start()

    nllbuf[0:4, :] = nll
    mine = nllbuf[pl.ds(b, 1), :]
    rolled = pltpu.roll(jnp.broadcast_to(mine, (8, 128)), lax.rem(128 - base, 128), 1)
    nll_out[...] = rolled[0:1, 0:4]

    rdma(abuf.at[:, 0:3], abuf.at[:, 0:3], asend, arecv.at[0, 0], partner).wait_send()
    rdma(wbuf.at[1], wbuf.at[1], wsend, wrecv.at[0], partner).wait_send()
    rdma(gath.at[:, 0, 0:7], gath.at[:, 0, 0:7], zsend, zrecv.at[0, 0], partner).wait_send()
    rdma(gath.at[:, 0:2], gath.at[:, 0:2], bsend, brecv.at[0, 0, 0], partner).wait_send()
    rdma(gath.at[:, 0], gath.at[:, 0], fsend, frecv.at[0, 0], partner).wait_send()

    swap.wait()
    sums = jnp.sum(last[0] + last[1], axis=1, keepdims=True)
    small = lax.broadcasted_iota(jnp.int32, (8, 8), 0) == lax.broadcasted_iota(jnp.int32, (8, 8), 1)
    for out, at in ((total_out, 0), (count_out, 8)):
        wide = jnp.where(small, jnp.broadcast_to(sums[at : at + 8, :], (8, 8)), 0.0)
        out[...] = jnp.sum(wide, axis=0, keepdims=True)


def zero_rows(acc, i):
    rows = pl.ds(pl.multiple_of(i * 64, 64), 64)
    for w in range(2):
        acc[w, rows, :] = jnp.zeros((64, acc.shape[2]), F32)


def body(hidden, lm_head, targets, segment, pad_mask, seq_bench):
    tok, width = hidden.shape
    voc = lm_head.shape[1]
    kp = width // PIECES
    tokens = GROUP * tok
    dma = pltpu.SemaphoreType.DMA
    anywhere = pl.BlockSpec(memory_space=pl.ANY)
    smem = pl.BlockSpec(memory_space=pltpu.SMEM)
    vmem = pl.BlockSpec(memory_space=pltpu.VMEM)
    nll, total, count = pl.pallas_call(
        kernel,
        out_shape=(
            jax.ShapeDtypeStruct((1, tok), F32),
            jax.ShapeDtypeStruct((1, NBENCH), F32),
            jax.ShapeDtypeStruct((1, NBENCH), F32),
        ),
        in_specs=[anywhere, anywhere, smem, smem, smem, smem],
        out_specs=(vmem, vmem, vmem),
        scratch_shapes=[
            pltpu.VMEM((PIECES, NA, tok, kp), jnp.bfloat16),
            pltpu.VMEM((NA * tok, kp), F32),
            pltpu.VMEM((PIECES, NB, NZ, NA * tok, kp), jnp.bfloat16),
            pltpu.VMEM((2, width, voc), jnp.bfloat16),
            pltpu.VMEM((2, tokens, voc), F32),
            pltpu.VMEM((tokens, 1), F32),
            pltpu.VMEM((NA + NB + NZ, 8, 128), F32),
            pltpu.VMEM((NA + NB + NZ, 8, 128), F32),
            pltpu.VMEM((2, 16, 128), F32),
            pltpu.VMEM((8, 128), F32),
            dma((PIECES,)), dma((PIECES,)), dma, dma((PIECES,)),
            dma, dma((PIECES, NA - 1)), dma, dma((PIECES, NZ - 1)),
            dma, dma((PIECES, 2, NZ)), dma, dma((PIECES, NZ)),
            dma((NA + NB + NZ,)), dma((NA + NB + NZ,)),
            dma((NA + NB + NZ,)), dma((NA + NB + NZ,)),
            dma, dma,
        ],
        compiler_params=pltpu.CompilerParams(
            collective_id=0, has_side_effects=True, vmem_limit_bytes=62 * 1024 * 1024
        ),
        name="nll",
    )(hidden, lm_head, targets, segment, pad_mask, seq_bench)
    return (nll.reshape(tok), total.reshape(NBENCH), count.reshape(NBENCH))


def solution(mesh):
    split = Mesh(mesh.devices.reshape(4, 2, 8, 4), AXES)
    return jax.shard_map(
        body,
        mesh=split,
        in_specs=(P(AXES, None), P(None, AXES), P(AXES), P(AXES), P(AXES), P()),
        out_specs=(P(AXES), P(), P()),
        check_vma=False,
    )
```

```python
import functools

import jax
import jax.numpy as jnp
from jax import lax
from jax.experimental import pallas as pl
from jax.experimental.pallas import tpu as pltpu
from jax.sharding import Mesh
from jax.sharding import PartitionSpec as P

NBENCH = 8
AXES = ("dp_0", "dp_1", "vocab_0", "vocab_1")
NA, NB, NZ = 4, 4, 8
PIECES = 8
LAG = 6
GROUP = NA * NB * NZ
DIST = (0, NZ - 1, 1, NZ - 2, 2, NZ - 3, 3, 4)
MESH = pl.DeviceIdType.MESH
F32 = jnp.float32


def kernel(
    hidden, weights, targets, segment, pad_mask, seq_bench,
    out,
    abuf, rows32, gath, wbuf, acc, info, stat, last, nllbuf,
    lsem, wlsem, wsend, wrecv, asend, arecv, zsend, zrecv,
    bsend, brecv, fsend, frecv, isend, irecv, ssend, srecv, csend, crecv,
):
    x, c = lax.axis_index("dp_0"), lax.axis_index("dp_1")
    z, y = lax.axis_index("vocab_0"), lax.axis_index("vocab_1")
    a = y * (1 - c) + x * c
    b = x * (1 - c) + y * c
    kp = abuf.shape[3]
    voc = weights.shape[0]

    def dev(a_, b_, z_, c_=None):
        if c_ is None:
            return (b_ * (1 - c) + a_ * c, c, z_, a_ * (1 - c) + b_ * c)
        return (x, c_, z, y)

    def rdma(src, dst, ssem, rsem, to):
        return pltpu.make_async_remote_copy(
            src_ref=src, dst_ref=dst, send_sem=ssem, recv_sem=rsem,
            device_id=to, device_id_type=MESH,
        )

    def a_at(k):
        return lax.rem(a + k, NA)

    def b_at(k):
        return lax.rem(b + k, NB)

    def z_at(k):
        return lax.rem(z + k, NZ)

    partner = dev(a, b, z, 1 - c)

    def own_hidden(p):
        cols = pl.ds(pl.multiple_of(p * kp, kp), kp)
        return pltpu.make_async_copy(hidden.at[:, cols], abuf.at[p, a], lsem.at[p])

    def own_weights(p):
        cols = pl.ds(pl.multiple_of(p * kp, kp), kp)
        return pltpu.make_async_copy(weights.at[:, cols], wbuf.at[0, :, cols], wlsem.at[p])

    def swap_weights(p):
        cols = pl.ds(pl.multiple_of(p * kp, kp), kp)
        return rdma(weights.at[:, cols], wbuf.at[1, :, cols], wsend, wrecv.at[p], partner)

    def loop(n, body):
        lax.fori_loop(0, n, lambda i, _: (body(i), 0)[1], 0)

    loop(PIECES, lambda p: own_hidden(p).start())

    barrier = pltpu.get_barrier_semaphore()
    peers = (
        [dev(a_at(k), b, z) for k in range(1, NA)]
        + [dev(a, b_at(k), z) for k in range(1, NB)]
        + [dev(a, b, z_at(k)) for k in range(1, NZ)]
        + [partner]
    )
    for peer in peers:
        pl.semaphore_signal(barrier, inc=1, device_id=peer, device_id_type=MESH)

    row = lax.broadcasted_iota(jnp.int32, (8, 128), 0)
    lane = lax.broadcasted_iota(jnp.int32, (8, 128), 1)
    base = z * (NA * 4) + a * 4
    own = jnp.zeros((8, 128), jnp.int32)
    whole_last = (x == NA - 1) & (c == 1) & (z == NZ - 1) & (y == NB - 1)
    for t in range(4):
        seg = segment[t]
        if t < 3:
            kept = (pad_mask[t] == 1) & (seg == segment[t + 1])
        else:
            kept = (pad_mask[t] == 1) & jnp.logical_not(whole_last)
        code = jnp.where(kept, seq_bench[seg], NBENCH)
        own = jnp.where((row == b) & (lane == base + t), targets[t], own)
        own = jnp.where((row == b + 4) & (lane == base + t), code, own)
    own = own.astype(F32)

    acc[...] = jnp.zeros(acc.shape, F32)

    pl.semaphore_wait(barrier, len(peers))

    def a_copy(p, k):
        return rdma(abuf.at[p, a], abuf.at[p, a], asend, arecv.at[p, k - 1], dev(a_at(k), b, z))

    def a_start(p):
        own_hidden(p).wait()
        for k in range(1, NA):
            a_copy(p, k).start()

    loop(PIECES, a_start)
    loop(PIECES, lambda p: own_weights(p).start())
    loop(PIECES, lambda p: swap_weights(p).start())

    def stage(buf, at, n, me, ssem, rsem, to, value):
        buf[at + me] = value
        for k in range(1, n):
            rdma(buf.at[at + me], buf.at[at + me], ssem.at[at + k], rsem.at[at + k], to(k)).start()

    def stage_wait(buf, at, n, me, ssem, rsem, to):
        for k in range(1, n):
            rdma(buf.at[at + me], buf.at[at + me], ssem.at[at + k], rsem.at[at + k], to(k)).wait()

    def to_a(k):
        return dev(a_at(k), b, z)

    def to_b(k):
        return dev(a, b_at(k), z)

    def to_z(k):
        return dev(a, b, z_at(k))

    sa, sb, sz = (0, NA, a, ), (NA, NB, b), (NA + NB, NZ, z)

    def added(buf, at, n):
        total = buf[at]
        for k in range(1, n):
            total = total + buf[at + k]
        return total

    stage(info, *sa, isend, irecv, to_a, own)

    def block(p, b_, z_):
        return gath.at[p, b_, z_]

    def z_copy(p, k, sem, up):
        zi = z_at(k)
        return rdma(block(p, b, zi), block(p, b, zi), zsend, zrecv.at[p, sem], dev(a, b, z_at(up)))

    def b_copy(p, j, way):
        zi = z_at(DIST[j])
        return rdma(
            block(p, b, zi), block(p, b, zi), bsend, brecv.at[p, way, j],
            dev(a, b_at(1 if way == 0 else NB - 1), z),
        )

    def f_copy(p, j):
        zi = z_at(DIST[j])
        come, go = (NB - 1, 1) if j % 2 == 0 else (1, NB - 1)
        return rdma(
            block(p, b_at(come), zi), block(p, b_at(come), zi), fsend, frecv.at[p, j],
            dev(a, b_at(go), z),
        )

    def b_both(p, j):
        b_copy(p, j, 0).start()
        b_copy(p, j, 1).start()

    def step_0(p):
        for k in range(1, NA):
            a_copy(p, k).wait_recv()
        for k in range(NA):
            rows32[4 * k : 4 * k + 4, :] = abuf[p, k].astype(F32)
        gath[p, b, z] = rows32[...].astype(jnp.bfloat16)
        z_copy(p, 0, 0, 1).start()
        z_copy(p, 0, 1, NZ - 1).start()
        b_both(p, 0)

    def step(p, s):
        z_copy(p, NZ - s, 2 * s - 2, 1).wait_recv()
        if s < 3:
            z_copy(p, NZ - s, 2 * s, 1).start()
        z_copy(p, s, 2 * s - 1, NZ - 1).wait_recv()
        if s < 3:
            z_copy(p, s, 2 * s + 1, NZ - 1).start()
        else:
            odd = lax.rem(p, 2)
            z_copy(p, 5 + 6 * odd, 6, 1 + 6 * odd).start()
        b_both(p, 2 * s - 1)
        b_both(p, 2 * s)

    def step_4(p):
        z_copy(p, 4, 6, 1).wait_recv()
        b_both(p, 7)

    def forward(p, s):
        for j in ((0,), (1, 2), (3, 4), (5, 6), (7,))[s]:
            b_copy(p, j, j % 2).wait_recv()
            f_copy(p, j).start()

    def multiply(p):
        for j in range(8):
            b_copy(p, j, 1 - j % 2).wait_recv()
            f_copy(p, j).wait_recv()
        own_weights(p).wait()
        swap_weights(p).wait_recv()
        cols = pl.ds(pl.multiple_of(p * kp, kp), kp)
        rows = gath[p].reshape(acc.shape[2], kp)
        for w in range(2):
            acc[w] += lax.dot_general(
                wbuf[w, :, cols], rows, (((1,), (1,)), ((), ())), preferred_element_type=F32
            )

    def at_piece(tick, lag, fn):
        p = tick - lag

        @pl.when((p >= 0) & (p < PIECES))
        def _():
            fn(p)

    def ticks(tick):
        at_piece(tick, 0, step_0)
        for s in range(1, 4):
            at_piece(tick, s, functools.partial(step, s=s))
        at_piece(tick, 4, step_4)
        for s in range(5):
            at_piece(tick, s + 1, functools.partial(forward, s=s))
        at_piece(tick, LAG, multiply)

        @pl.when(tick == 2)
        def _():
            stage_wait(info, *sa, isend, irecv, to_a)
            stage(info, *sb, isend, irecv, to_b, added(info, 0, NA))

        @pl.when(tick == 4)
        def _():
            stage_wait(info, *sb, isend, irecv, to_b)
            stage(info, *sz, isend, irecv, to_z, added(info, NA, NB))

        @pl.when(tick == 6)
        def _():
            stage_wait(info, *sz, isend, irecv, to_z)
            info[0] = added(info, NA + NB, NZ)

    loop(PIECES + LAG, ticks)

    index = ((x * 2 + c) * NZ + z) * NB + y
    other = ((x * 2 + 1 - c) * NZ + z) * NB + y
    entries = lax.broadcasted_iota(jnp.int32, (voc, 128), 0)
    numbers = [(entries + i * voc).astype(F32) for i in (index, other)]
    for k in range(4):
        cols = slice(k * 128, (k + 1) * 128)
        logits = [acc[w, :, cols] for w in range(2)]
        wanted = info[0, k : k + 1, :]
        tops = [jnp.max(part, axis=0, keepdims=True) for part in logits]
        top = jnp.maximum(*tops)
        total = sum(jnp.sum(jnp.exp(part - top), axis=0, keepdims=True) for part in logits)
        picked = sum(
            jnp.sum(jnp.where(number == wanted, part, 0.0), axis=0, keepdims=True)
            for number, part in zip(numbers, logits)
        )
        nllbuf[k : k + 1, :] = top + jnp.log(total)
        nllbuf[k + 4 : k + 5, :] = picked

    def merged(buf, at, n):
        parts = [buf[at + k] for k in range(n)]
        top = functools.reduce(jnp.maximum, parts)
        total = functools.reduce(jnp.add, [jnp.exp(part - top) for part in parts])
        picked = functools.reduce(jnp.add, parts)
        return jnp.where(row < 4, top + jnp.log(total), picked)

    stage(stat, *sa, ssend, srecv, to_a, nllbuf[...])
    stage_wait(stat, *sa, ssend, srecv, to_a)
    stage(stat, *sb, ssend, srecv, to_b, merged(stat, 0, NA))
    stage_wait(stat, *sb, ssend, srecv, to_b)
    stage(stat, *sz, ssend, srecv, to_z, merged(stat, NA, NB))
    stage_wait(stat, *sz, ssend, srecv, to_z)
    both = merged(stat, NA + NB, NZ)
    nll = both[0:4, :] - both[4:8, :]

    codes = info[0][4:8, :]
    last_t, last_c = jnp.zeros((8, 128), F32), jnp.zeros((8, 128), F32)
    for j in range(NBENCH):
        hit = codes == float(j)
        part_t = jnp.sum(jnp.where(hit, nll, 0.0), axis=0, keepdims=True)
        part_c = jnp.sum(jnp.where(hit, 1.0, 0.0), axis=0, keepdims=True)
        last_t = jnp.where(row == j, part_t, last_t)
        last_c = jnp.where(row == j, part_c, last_c)
    last[c, 0:8, :] = last_t
    last[c, 8:16, :] = last_c
    swap = rdma(last.at[c], last.at[c], csend, crecv, partner)
    swap.start()

    nllbuf[0:4, :] = nll
    mine = nllbuf[pl.ds(b, 1), :]
    rolled = pltpu.roll(jnp.broadcast_to(mine, (8, 128)), lax.rem(128 - base, 128), 1)

    rdma(abuf.at[:, 0:3], abuf.at[:, 0:3], asend, arecv.at[0, 0], partner).wait_send()
    rdma(weights, wbuf.at[1], wsend, wrecv.at[0], partner).wait_send()
    rdma(gath.at[:, 0, 0:7], gath.at[:, 0, 0:7], zsend, zrecv.at[0, 0], partner).wait_send()
    rdma(gath.at[:, 0:2], gath.at[:, 0:2], bsend, brecv.at[0, 0, 0], partner).wait_send()
    rdma(gath.at[:, 0], gath.at[:, 0], fsend, frecv.at[0, 0], partner).wait_send()

    swap.wait()
    sums = jnp.sum(last[0] + last[1], axis=1, keepdims=True)
    row16 = lax.broadcasted_iota(jnp.int32, (16, 128), 0)
    lane16 = lax.broadcasted_iota(jnp.int32, (16, 128), 1)
    sums = jnp.sum(jnp.where(lane16 == row16 + 4, sums, 0.0), axis=0, keepdims=True)
    out[...] = jnp.where(lane[0:1, :] < 4, rolled[0:1, :], sums)


def body(hidden, lm_head, targets, segment, pad_mask, seq_bench):
    tok, width = hidden.shape
    voc = lm_head.shape[1]
    kp = width // PIECES
    tokens = GROUP * tok
    dma = pltpu.SemaphoreType.DMA
    anywhere = pl.BlockSpec(memory_space=pl.ANY)
    smem = pl.BlockSpec(memory_space=pltpu.SMEM)
    vmem = pl.BlockSpec(memory_space=pltpu.VMEM)
    out = pl.pallas_call(
        kernel,
        out_shape=jax.ShapeDtypeStruct((1, 128), F32),
        in_specs=[anywhere, anywhere, smem, smem, smem, smem],
        out_specs=vmem,
        scratch_shapes=[
            pltpu.VMEM((PIECES, NA, tok, kp), jnp.bfloat16),
            pltpu.VMEM((NA * tok, kp), F32),
            pltpu.VMEM((PIECES, NB, NZ, NA * tok, kp), jnp.bfloat16),
            pltpu.VMEM((2, voc, width), jnp.bfloat16),
            pltpu.VMEM((2, voc, tokens), F32),
            pltpu.VMEM((NA + NB + NZ, 8, 128), F32),
            pltpu.VMEM((NA + NB + NZ, 8, 128), F32),
            pltpu.VMEM((2, 16, 128), F32),
            pltpu.VMEM((8, 128), F32),
            dma((PIECES,)), dma((PIECES,)), dma, dma((PIECES,)),
            dma, dma((PIECES, NA - 1)), dma, dma((PIECES, NZ - 1)),
            dma, dma((PIECES, 2, NZ)), dma, dma((PIECES, NZ)),
            dma((NA + NB + NZ,)), dma((NA + NB + NZ,)),
            dma((NA + NB + NZ,)), dma((NA + NB + NZ,)),
            dma, dma,
        ],
        compiler_params=pltpu.CompilerParams(
            collective_id=0, has_side_effects=True, vmem_limit_bytes=62 * 1024 * 1024
        ),
        name="nll",
    )(hidden, lm_head.T, targets, segment, pad_mask, seq_bench)
    line = out[0]
    return (line[:tok], line[tok : tok + NBENCH], line[tok + NBENCH : tok + 2 * NBENCH])


def solution(mesh):
    split = Mesh(mesh.devices.reshape(4, 2, 8, 4), AXES)
    return jax.shard_map(
        body,
        mesh=split,
        in_specs=(P(AXES, None), P(None, AXES), P(AXES), P(AXES), P(AXES), P()),
        out_specs=(P(AXES), P(), P()),
        check_vma=False,
    )
```

```python
import functools

import jax
import jax.numpy as jnp
from jax import lax
from jax.experimental import pallas as pl
from jax.experimental.pallas import tpu as pltpu
from jax.sharding import Mesh
from jax.sharding import PartitionSpec as P

NBENCH = 8
AXES = ("dp_0", "dp_1", "vocab_0", "vocab_1")
NA, NB, NZ = 4, 4, 8
PIECES = 8
LAST = PIECES - 1
LAG = 6
GROUP = NA * NB * NZ
DIST = (0, NZ - 1, 1, NZ - 2, 2, NZ - 3, 3, 4)
MESH = pl.DeviceIdType.MESH
F32 = jnp.float32


def kernel(
    hidden, weights, targets, segment, pad_mask, seq_bench,
    out,
    tgt_s, seg_s, pad_s, ben_s,
    abuf, rows32, gath, wbuf, acc, info, stat, last, nllbuf,
    small, lsem, wlsem, wsend, wrecv, asend, arecv, zsend, zrecv,
    bsend, brecv, fsend, frecv, ebsend, ebrecv, ezsend, ezrecv,
    isend, irecv, ssend, srecv, csend, crecv,
):
    x, c = lax.axis_index("dp_0"), lax.axis_index("dp_1")
    z, y = lax.axis_index("vocab_0"), lax.axis_index("vocab_1")
    a = y * (1 - c) + x * c
    b = x * (1 - c) + y * c
    kp = abuf.shape[3]
    voc = weights.shape[0]

    def dev(a_, b_, z_):
        return (b_ * (1 - c) + a_ * c, c, z_, a_ * (1 - c) + b_ * c)

    def rdma(src, dst, ssem, rsem, to):
        return pltpu.make_async_remote_copy(
            src_ref=src, dst_ref=dst, send_sem=ssem, recv_sem=rsem,
            device_id=to, device_id_type=MESH,
        )

    def a_at(k):
        return lax.rem(a + k, NA)

    def b_at(k):
        return lax.rem(b + k, NB)

    def z_at(k):
        return lax.rem(z + k, NZ)

    partner = (x, 1 - c, z, y)

    def columns(p):
        return pl.ds(pl.multiple_of(p * kp, kp), kp)

    def own_hidden(p):
        return pltpu.make_async_copy(hidden.at[:, columns(p)], abuf.at[p, a], lsem.at[p])

    def own_weights(p):
        cols = columns(p)
        return pltpu.make_async_copy(weights.at[:, cols], wbuf.at[0, :, cols], wlsem.at[p])

    def swap_weights(p):
        cols = columns(p)
        return rdma(weights.at[:, cols], wbuf.at[1, :, cols], wsend, wrecv.at[p], partner)

    def loop(n, fn):
        lax.fori_loop(0, n, lambda i, _: (fn(i), 0)[1], 0)

    def turn(i):
        return lax.rem(i + LAST, PIECES)

    loop(PIECES, lambda i: own_hidden(turn(i)).start())
    smalls = [
        pltpu.make_async_copy(src, dst, small.at[k])
        for k, (src, dst) in enumerate(
            ((targets, tgt_s), (segment, seg_s), (pad_mask, pad_s), (seq_bench, ben_s))
        )
    ]
    for copy in smalls:
        copy.start()

    barrier = pltpu.get_barrier_semaphore()
    peers = [dev(a_at(k), b, z) for k in range(1, NA)]
    peers += [dev(a, b_at(k), z) for k in (1, NB - 1)]
    peers += [dev(a, b, z_at(k)) for k in (1, NZ - 1)]
    peers += [partner]
    for peer in peers:
        pl.semaphore_signal(barrier, inc=1, device_id=peer, device_id_type=MESH)
    pl.semaphore_wait(barrier, len(peers))

    def a_copy(p, k):
        return rdma(abuf.at[p, a], abuf.at[p, a], asend, arecv.at[p, k - 1], dev(a_at(k), b, z))

    def a_start(i):
        p = turn(i)
        own_hidden(p).wait()
        for k in range(1, NA):
            a_copy(p, k).start()

    loop(PIECES, a_start)
    loop(PIECES, lambda p: own_weights(p).start())
    loop(PIECES, lambda p: swap_weights(p).start())
    acc[...] = jnp.zeros(acc.shape, F32)

    def planes(buf, ssem, rsem):
        at = a * NB + b
        return [
            rdma(buf.at[at], buf.at[at], ssem.at[k], rsem.at[k], dev(a_at(k // NB), b_at(k % NB), z))
            for k in range(1, NA * NB)
        ]

    def lines(buf, ssem, rsem):
        at = NA * NB + z
        return [
            rdma(
                buf.at[at], buf.at[at], ssem.at[NA * NB + k], rsem.at[NA * NB + k],
                dev(a, b, z_at(k)),
            )
            for k in range(1, NZ)
        ]

    def start_all(copies):
        for copy in copies:
            copy.start()

    def wait_all(copies):
        for copy in copies:
            copy.wait()

    def added(buf, at, n):
        total = buf[at]
        for k in range(1, n):
            total = total + buf[at + k]
        return total

    def block(p, b_, z_):
        return gath.at[p, z_, b_]

    def z_copy(p, b_, k, ssem, rsem, up):
        zi = z_at(k)
        return rdma(block(p, b_, zi), block(p, b_, zi), ssem, rsem, dev(a, b, z_at(up)))

    def b_send(p, zi, b_, ssem, rsem, go):
        return rdma(block(p, b_, zi), block(p, b_, zi), ssem, rsem, dev(a, b_at(go), z))

    def b_copy(p, j, way):
        go = 1 if way == 0 else NB - 1
        return b_send(p, z_at(DIST[j]), b, bsend, brecv.at[p, way, j], go)

    def f_copy(p, j):
        come, go = (NB - 1, 1) if j % 2 == 0 else (1, NB - 1)
        return b_send(p, z_at(DIST[j]), b_at(come), fsend, frecv.at[p, j], go)

    def b_both(p, j):
        b_copy(p, j, 0).start()
        b_copy(p, j, 1).start()

    def tile_rows(p):
        for k in range(1, NA):
            a_copy(p, k).wait_recv()
        for k in range(NA):
            rows32[4 * k : 4 * k + 4, :] = abuf[p, k].astype(F32)
        gath[p, z, b] = rows32[...].astype(jnp.bfloat16)

    def e_copy(k, src, go):
        return b_send(LAST, z, b_at(src), ebsend, ebrecv.at[k], go)

    tile_rows(LAST)
    e_copy(0, 0, 1).start()
    e_copy(1, 0, NB - 1).start()

    def begin(p):
        tile_rows(p)
        b_both(p, 0)

        @pl.when(p == 0)
        def _():
            z_step(p, 0, p, b, zsend, zrecv)

    def z_step(p, s, u, b_, ssem, rsem):
        if s == 0:
            z_copy(p, b_, 0, ssem, rsem.at[u, 0], 1).start()
            z_copy(p, b_, 0, ssem, rsem.at[u, 1], NZ - 1).start()
        elif s < 4:
            odd = lax.rem(u, 2)
            z_copy(p, b_, NZ - s, ssem, rsem.at[u, 2 * s - 2], 1).wait_recv()
            if s < 3:
                z_copy(p, b_, NZ - s, ssem, rsem.at[u, 2 * s], 1).start()
            z_copy(p, b_, s, ssem, rsem.at[u, 2 * s - 1], NZ - 1).wait_recv()
            if s < 3:
                z_copy(p, b_, s, ssem, rsem.at[u, 2 * s + 1], NZ - 1).start()
            else:
                z_copy(p, b_, 5 + 6 * odd, ssem, rsem.at[u, 6], 1 + 6 * odd).start()
        else:
            z_copy(p, b_, 4, ssem, rsem.at[u, 6], 1).wait_recv()

    loop(LAST, begin)

    def step(p, s):
        z_step(p, s, p, b, zsend, zrecv)
        if 0 < s < 4:
            b_both(p, 2 * s - 1)
            b_both(p, 2 * s)
        elif s == 4:
            b_both(p, 7)

    def e_step(u, s):
        b_ = b_at(u + (u // 2) * (5 - 2 * u))
        z_step(LAST, s, u, b_, ezsend, ezrecv)

    def forward(p, s):
        for j in ((0,), (1, 2), (3, 4), (5, 6), (7,))[s]:
            b_copy(p, j, j % 2).wait_recv()
            f_copy(p, j).start()

    def product(p):
        own_weights(p).wait()
        swap_weights(p).wait_recv()
        cols = columns(p)
        rows = gath[p].reshape(acc.shape[2], kp)
        for w in range(2):
            acc[w] += lax.dot_general(
                wbuf[w, :, cols], rows, (((1,), (1,)), ((), ())), preferred_element_type=F32
            )

    def multiply(p):
        @pl.when(p < LAST)
        def _():
            for j in range(8):
                b_copy(p, j, 1 - j % 2).wait_recv()
                f_copy(p, j).wait_recv()

        product(p)

    def at_piece(tick, lag, fn):
        p = tick - lag

        @pl.when((p >= 0) & (p < LAST))
        def _():
            fn(p)

    row = lax.broadcasted_iota(jnp.int32, (8, 128), 0)
    lane = lax.broadcasted_iota(jnp.int32, (8, 128), 1)
    base = b * 16 + a * 4

    def own_info():
        own = jnp.zeros((8, 128), jnp.int32)
        whole_last = (x == NA - 1) & (c == 1) & (z == NZ - 1) & (y == NB - 1)
        for t in range(4):
            seg = seg_s[t]
            if t < 3:
                kept = (pad_s[t] == 1) & (seg == seg_s[t + 1])
            else:
                kept = (pad_s[t] == 1) & jnp.logical_not(whole_last)
            code = jnp.where(kept, ben_s[seg], NBENCH)
            own = jnp.where((row == z) & (lane == base + t), tgt_s[t], own)
            own = jnp.where((row == z) & (lane == base + t + 64), code, own)
        return own.astype(F32)

    def ticks(tick):
        @pl.when(tick > 0)
        def _():
            at_piece(tick, 0, functools.partial(step, s=0))

        for s in range(1, 5):
            at_piece(tick, s, functools.partial(step, s=s))

        @pl.when(tick == 1)
        def _():
            e_copy(0, 0, 1).wait_recv()
            e_copy(1, 0, NB - 1).wait_recv()
            e_copy(2, NB - 1, 1).start()

        @pl.when(tick == 3)
        def _():
            e_copy(2, NB - 1, 1).wait_recv()

        for s in range(5):
            at_piece(tick, s + 1, functools.partial(forward, s=s))

        for s in range(5):
            twice = tick - 1 - s

            @pl.when((twice >= 0) & (twice < 2 * NB) & (lax.rem(twice, 2) == 0))
            def _():
                e_step(twice // 2, s)

        @pl.when((tick >= LAG) & (tick < LAG + LAST - 1))
        def _():
            multiply(tick - LAG)

        @pl.when(tick == 7)
        def _():
            wait_all(smalls)
            info[a * NB + b] = own_info()
            start_all(planes(info, isend, irecv))

        @pl.when(tick == 9)
        def _():
            wait_all(planes(info, isend, irecv))
            info[NA * NB + z] = added(info, 0, NA * NB)
            start_all(lines(info, isend, irecv))

        @pl.when(tick == 11)
        def _():
            wait_all(lines(info, isend, irecv))
            info[0] = added(info, NA * NB, NZ)

    loop(LAG + LAST - 1, ticks)
    loop(2, lambda i: multiply(LAST - i))

    index = ((x * 2 + c) * NZ + z) * NB + y
    other = ((x * 2 + 1 - c) * NZ + z) * NB + y
    entries = lax.broadcasted_iota(jnp.int32, (voc, 128), 0)
    numbers = [(entries + i * voc).astype(F32) for i in (index, other)]
    left = lane[0:1, :] < 64
    every = info[0]

    def over(line):
        return pltpu.roll(jnp.broadcast_to(line, (8, 128)), 64, 1)[0:1, :]

    for k in range(4):
        cols = slice(k * 128, (k + 1) * 128)
        logits = [acc[w, :, cols] for w in range(2)]
        wanted = jnp.where(left, every[2 * k : 2 * k + 1, :], over(every[2 * k + 1 : 2 * k + 2, :]))
        tops = [jnp.max(part, axis=0, keepdims=True) for part in logits]
        top = jnp.maximum(*tops)
        total = sum(jnp.sum(jnp.exp(part - top), axis=0, keepdims=True) for part in logits)
        picked = sum(
            jnp.sum(jnp.where(number == wanted, part, 0.0), axis=0, keepdims=True)
            for number, part in zip(numbers, logits)
        )
        lse = top + jnp.log(total)
        nllbuf[2 * k : 2 * k + 1, :] = jnp.where(left, lse, over(picked))
        nllbuf[2 * k + 1 : 2 * k + 2, :] = jnp.where(left, over(lse), picked)

    def merged(buf, at, n):
        parts = [buf[at + k] for k in range(n)]
        top = functools.reduce(jnp.maximum, parts)
        total = functools.reduce(jnp.add, [jnp.exp(part - top) for part in parts])
        picked = functools.reduce(jnp.add, parts)
        return jnp.where(lane < 64, top + jnp.log(total), picked)

    stat[a * NB + b] = nllbuf[...]
    start_all(planes(stat, ssend, srecv))
    wait_all(planes(stat, ssend, srecv))
    stat[NA * NB + z] = merged(stat, 0, NA * NB)
    start_all(lines(stat, ssend, srecv))
    wait_all(lines(stat, ssend, srecv))
    both = merged(stat, NA * NB, NZ)
    nll = both - pltpu.roll(both, 64, 1)

    codes = jnp.where(lane < 64, pltpu.roll(every, 64, 1), float(NBENCH))
    last_t, last_c = jnp.zeros((8, 128), F32), jnp.zeros((8, 128), F32)
    for j in range(NBENCH):
        hit = codes == float(j)
        part_t = jnp.sum(jnp.where(hit, nll, 0.0), axis=0, keepdims=True)
        part_c = jnp.sum(jnp.where(hit, 1.0, 0.0), axis=0, keepdims=True)
        last_t = jnp.where(row == j, part_t, last_t)
        last_c = jnp.where(row == j, part_c, last_c)
    last[c, 0:8, :] = last_t
    last[c, 8:16, :] = last_c
    swap = rdma(last.at[c], last.at[c], csend, crecv, partner)
    swap.start()

    nllbuf[...] = nll
    mine = nllbuf[pl.ds(z, 1), :]
    rolled = pltpu.roll(jnp.broadcast_to(mine, (8, 128)), lax.rem(128 - base, 128), 1)

    def left_all(ref, ssem, rsem):
        rdma(ref, ref, ssem, rsem, partner).wait_send()

    left_all(abuf.at[:, 0:3], asend, arecv.at[0, 0])
    rdma(weights, wbuf.at[1], wsend, wrecv.at[0], partner).wait_send()
    left_all(gath.at[0:LAST, 0:7, 0], zsend, zrecv.at[0, 0])
    left_all(gath.at[0:LAST, 0:4], bsend, brecv.at[0, 0, 0])
    left_all(gath.at[0:LAST, 0:2], fsend, frecv.at[0, 0])
    left_all(gath.at[LAST, 0, 0:3], ebsend, ebrecv.at[0])
    left_all(gath.at[LAST, 0:7], ezsend, ezrecv.at[0, 0])

    swap.wait()
    sums = jnp.sum(last[0] + last[1], axis=1, keepdims=True)
    row16 = lax.broadcasted_iota(jnp.int32, (16, 128), 0)
    lane16 = lax.broadcasted_iota(jnp.int32, (16, 128), 1)
    sums = jnp.sum(jnp.where(lane16 == row16 + 4, sums, 0.0), axis=0, keepdims=True)
    out[...] = jnp.where(lane[0:1, :] < 4, rolled[0:1, :], sums)


def body(hidden, lm_head, targets, segment, pad_mask, seq_bench):
    tok, width = hidden.shape
    voc = lm_head.shape[1]
    kp = width // PIECES
    tokens = GROUP * tok
    dma = pltpu.SemaphoreType.DMA
    anywhere = pl.BlockSpec(memory_space=pl.ANY)
    vmem = pl.BlockSpec(memory_space=pltpu.VMEM)
    out = pl.pallas_call(
        kernel,
        out_shape=jax.ShapeDtypeStruct((1, 128), F32),
        in_specs=[anywhere] * 6,
        out_specs=vmem,
        scratch_shapes=[
            pltpu.SMEM((tok,), jnp.int32),
            pltpu.SMEM((tok,), jnp.int32),
            pltpu.SMEM((tok,), jnp.int32),
            pltpu.SMEM(seq_bench.shape, jnp.int32),
            pltpu.VMEM((PIECES, NA, tok, kp), jnp.bfloat16),
            pltpu.VMEM((NA * tok, kp), F32),
            pltpu.VMEM((PIECES, NZ, NB, NA * tok, kp), jnp.bfloat16),
            pltpu.VMEM((2, voc, width), jnp.bfloat16),
            pltpu.VMEM((2, voc, tokens), F32),
            pltpu.VMEM((NA * NB + NZ, 8, 128), F32),
            pltpu.VMEM((NA * NB + NZ, 8, 128), F32),
            pltpu.VMEM((2, 16, 128), F32),
            pltpu.VMEM((8, 128), F32),
            dma((4,)), dma((PIECES,)), dma((PIECES,)), dma, dma((PIECES,)),
            dma, dma((PIECES, NA - 1)), dma, dma((LAST, NZ - 1)),
            dma, dma((LAST, 2, NZ)), dma, dma((LAST, NZ)),
            dma, dma((3,)), dma, dma((NB, NZ - 1)),
            dma((NA * NB + NZ,)), dma((NA * NB + NZ,)),
            dma((NA * NB + NZ,)), dma((NA * NB + NZ,)),
            dma, dma,
        ],
        compiler_params=pltpu.CompilerParams(
            collective_id=0, has_side_effects=True, vmem_limit_bytes=62 * 1024 * 1024
        ),
        name="nll",
    )(hidden, lm_head.T, targets, segment, pad_mask, seq_bench)
    line = out[0]
    return (line[:tok], line[tok : tok + NBENCH], line[tok + NBENCH : tok + 2 * NBENCH])


def solution(mesh):
    split = Mesh(mesh.devices.reshape(4, 2, 8, 4), AXES)
    return jax.shard_map(
        body,
        mesh=split,
        in_specs=(P(AXES, None), P(None, AXES), P(AXES), P(AXES), P(AXES), P()),
        out_specs=(P(AXES), P(), P()),
        check_vma=False,
    )
```

```python
import functools

import jax
import jax.numpy as jnp
from jax import lax
from jax.experimental import pallas as pl
from jax.experimental.pallas import tpu as pltpu
from jax.sharding import Mesh
from jax.sharding import PartitionSpec as P

NBENCH = 8
AXES = ("dp_0", "dp_1", "vocab_0", "vocab_1")
NA, NB, NZ = 4, 4, 8
PIECES = 8
LAST = PIECES - 1
GROUP = NA * NB * NZ
PLAN = {
    (1, 3): [(0, 0)], (1, 5): [(1, 0)], (1, 6): [(2, 0)], (2, 0): [(3, 0)], (2, 3): [(0, 1)],
    (3, 0): [(1, 1)], (3, 1): [(2, 1)], (3, 4): [(3, 1)],
    (4, 1): [(0, 2), (1, 2)], (4, 2): [(2, 2)], (4, 3): [(3, 2)], (4, 5): [(0, 3)],
    (4, 6): [(1, 3)], (4, 7): [(2, 3), (3, 3)], (4, 8): [(0, 4), (1, 4), (2, 4), (3, 4)],
}
MESH = pl.DeviceIdType.MESH
F32 = jnp.float32


def kernel(
    hidden, weights, targets, segment, pad_mask, seq_bench,
    out,
    tgt_s, seg_s, pad_s, ben_s,
    abuf, rows32, gath, wbuf, acc, info, stat, last, nllbuf,
    small, lsem, wlsem, wsend, wrecv, asend, arecv, zsend, zrecv,
    bsend, brecv, fsend, frecv, ebsend, ebrecv, ezsend, ezrecv,
    isend, irecv, ssend, srecv, csend, crecv,
):
    x, c = lax.axis_index("dp_0"), lax.axis_index("dp_1")
    z, y = lax.axis_index("vocab_0"), lax.axis_index("vocab_1")
    a = y * (1 - c) + x * c
    b = x * (1 - c) + y * c
    kp = abuf.shape[3]
    voc = weights.shape[0]

    def dev(a_, b_, z_):
        return (b_ * (1 - c) + a_ * c, c, z_, a_ * (1 - c) + b_ * c)

    def rdma(src, dst, ssem, rsem, to):
        return pltpu.make_async_remote_copy(
            src_ref=src, dst_ref=dst, send_sem=ssem, recv_sem=rsem,
            device_id=to, device_id_type=MESH,
        )

    def a_at(k):
        return lax.rem(a + k, NA)

    def b_at(k):
        return lax.rem(b + k, NB)

    def z_at(k):
        return lax.rem(z + k, NZ)

    partner = (x, 1 - c, z, y)

    def columns(p):
        return pl.ds(pl.multiple_of(p * kp, kp), kp)

    def own_hidden(p):
        return pltpu.make_async_copy(hidden.at[:, columns(p)], abuf.at[p, a], lsem.at[p])

    def own_weights(p):
        cols = columns(p)
        return pltpu.make_async_copy(weights.at[:, cols], wbuf.at[0, :, cols], wlsem.at[p])

    def swap_weights(p):
        cols = columns(p)
        return rdma(weights.at[:, cols], wbuf.at[1, :, cols], wsend, wrecv.at[p], partner)

    def loop(n, fn):
        lax.fori_loop(0, n, lambda i, _: (fn(i), 0)[1], 0)

    def turn(i):
        return lax.rem(i + LAST, PIECES)

    loop(PIECES, lambda i: own_hidden(turn(i)).start())
    smalls = [
        pltpu.make_async_copy(src, dst, small.at[k])
        for k, (src, dst) in enumerate(
            ((targets, tgt_s), (segment, seg_s), (pad_mask, pad_s), (seq_bench, ben_s))
        )
    ]
    for copy in smalls:
        copy.start()

    barrier = pltpu.get_barrier_semaphore()
    peers = [dev(a_at(k), b, z) for k in range(1, NA)]
    peers += [dev(a, b_at(k), z) for k in (1, NB - 1)]
    peers += [dev(a, b, z_at(k)) for k in (1, NZ - 1)]
    peers += [partner]
    for peer in peers:
        pl.semaphore_signal(barrier, inc=1, device_id=peer, device_id_type=MESH)
    pl.semaphore_wait(barrier, len(peers))

    def a_copy(p, k):
        return rdma(abuf.at[p, a], abuf.at[p, a], asend, arecv.at[p, k - 1], dev(a_at(k), b, z))

    def a_start(i):
        p = turn(i)
        own_hidden(p).wait()
        for k in range(1, NA):
            a_copy(p, k).start()

    loop(PIECES, a_start)
    loop(PIECES, lambda p: own_weights(p).start())
    loop(PIECES, lambda p: swap_weights(p).start())
    acc[...] = jnp.zeros(acc.shape, F32)

    def planes(buf, ssem, rsem):
        at = a * NB + b
        return [
            rdma(buf.at[at], buf.at[at], ssem.at[k], rsem.at[k], dev(a_at(k // NB), b_at(k % NB), z))
            for k in range(1, NA * NB)
        ]

    def lines(buf, ssem, rsem):
        at = NA * NB + z
        return [
            rdma(
                buf.at[at], buf.at[at], ssem.at[NA * NB + k], rsem.at[NA * NB + k],
                dev(a, b, z_at(k)),
            )
            for k in range(1, NZ)
        ]

    def start_all(copies):
        for copy in copies:
            copy.start()

    def wait_all(copies):
        for copy in copies:
            copy.wait()

    def added(buf, at, n):
        total = buf[at]
        for k in range(1, n):
            total = total + buf[at + k]
        return total

    def dist(j, odd=None):
        odd = j % 2 if odd is None else odd
        return NZ - 1 - j // 2 if odd else j // 2

    def block(p, b_, z_):
        return gath.at[p, z_, b_]

    def z_copy(p, b_, k, ssem, rsem, up):
        zi = z_at(k)
        return rdma(block(p, b_, zi), block(p, b_, zi), ssem, rsem, dev(a, b, z_at(up)))

    def b_send(p, zi, b_, ssem, rsem, go):
        return rdma(block(p, b_, zi), block(p, b_, zi), ssem, rsem, dev(a, b_at(go), z))

    def b_copy(p, j, way, odd=None):
        go = 1 if way == 0 else NB - 1
        return b_send(p, z_at(dist(j, odd)), b, bsend, brecv.at[p, way, j], go)

    def f_copy(p, j, odd=None):
        odd = j % 2 if odd is None else odd
        come, go = (1, NB - 1) if odd else (NB - 1, 1)
        return b_send(p, z_at(dist(j, odd)), b_at(come), fsend, frecv.at[p, j], go)

    def b_both(p, j):
        b_copy(p, j, 0).start()
        b_copy(p, j, 1).start()

    def tile_rows(p):
        for k in range(1, NA):
            a_copy(p, k).wait_recv()
        for k in range(NA):
            rows32[4 * k : 4 * k + 4, :] = abuf[p, k].astype(F32)
        gath[p, z, b] = rows32[...].astype(jnp.bfloat16)

    def e_copy(k, src, go):
        return b_send(LAST, z, b_at(src), ebsend, ebrecv.at[k], go)

    tile_rows(LAST)
    e_copy(0, 0, 1).start()
    e_copy(1, 0, NB - 1).start()

    def begin(p):
        tile_rows(p)
        b_both(p, 0)

        z_step(p, 0, p, b, zsend, zrecv)

    def z_step(p, s, u, b_, ssem, rsem):
        if s == 0:
            z_copy(p, b_, 0, ssem, rsem.at[u, 0], 1).start()
            z_copy(p, b_, 0, ssem, rsem.at[u, 1], NZ - 1).start()
        elif s < 4:
            odd = lax.rem(u, 2)
            z_copy(p, b_, NZ - s, ssem, rsem.at[u, 2 * s - 2], 1).wait_recv()
            if s < 3:
                z_copy(p, b_, NZ - s, ssem, rsem.at[u, 2 * s], 1).start()
            z_copy(p, b_, s, ssem, rsem.at[u, 2 * s - 1], NZ - 1).wait_recv()
            if s < 3:
                z_copy(p, b_, s, ssem, rsem.at[u, 2 * s + 1], NZ - 1).start()
            else:
                z_copy(p, b_, 5 + 6 * odd, ssem, rsem.at[u, 6], 1 + 6 * odd).start()
        else:
            z_copy(p, b_, 4, ssem, rsem.at[u, 6], 1).wait_recv()

    loop(LAST, begin)

    def step(p, s):
        z_step(p, s, p, b, zsend, zrecv)
        if 0 < s < 4:
            b_both(p, 2 * s - 1)
            b_both(p, 2 * s)
        elif s == 4:
            b_both(p, 7)

    def e_step(u, s):
        b_ = b_at(u + (u // 2) * (5 - 2 * u))
        z_step(LAST, s, u, b_, ezsend, ezrecv)

    def forward(p, s):
        for j in ((0,), (1, 2), (3, 4), (5, 6), (7,))[s]:
            b_copy(p, j, j % 2).wait_recv()
            f_copy(p, j).start()

    def multiply(p, h):
        @pl.when(p < LAST)
        def _():
            for k in range(4):
                b_copy(p, 4 * h + k, 1 - k % 2, k % 2).wait_recv()
                f_copy(p, 4 * h + k, k % 2).wait_recv()

        @pl.when(h == 0)
        def _():
            own_weights(p).wait()
            swap_weights(p).wait_recv()

        cols = columns(p)
        rows = jnp.concatenate(
            [gath[p, z_at(dist(4 * h + k, k % 2))].reshape(NB * 16, kp) for k in range(4)], axis=0
        )
        for w in range(2):
            acc[h, w] += lax.dot_general(
                wbuf[w, :, cols], rows, (((1,), (1,)), ((), ())), preferred_element_type=F32
            )

    row = lax.broadcasted_iota(jnp.int32, (8, 128), 0)
    lane = lax.broadcasted_iota(jnp.int32, (8, 128), 1)
    base = b * 16 + a * 4

    def own_info():
        own = jnp.zeros((8, 128), jnp.int32)
        whole_last = (x == NA - 1) & (c == 1) & (z == NZ - 1) & (y == NB - 1)
        for t in range(4):
            seg = seg_s[t]
            if t < 3:
                kept = (pad_s[t] == 1) & (seg == seg_s[t + 1])
            else:
                kept = (pad_s[t] == 1) & jnp.logical_not(whole_last)
            code = jnp.where(kept, ben_s[seg], NBENCH)
            own = jnp.where((row == z) & (lane == base + t), tgt_s[t], own)
            own = jnp.where((row == z) & (lane == base + t + 64), code, own)
        return own.astype(F32)

    def planned(s, i, count):
        for at in range(count):
            if (s, at) in PLAN:

                @pl.when(i == at)
                def _():
                    for u, k in PLAN[s, at]:
                        e_step(u, k)

    def level(s, p):
        if s == 1:

            @pl.when(p == 0)
            def _():
                e_copy(0, 0, 1).wait_recv()
                e_copy(1, 0, NB - 1).wait_recv()
                e_copy(2, NB - 1, 1).start()

            @pl.when(p == 6)
            def _():
                e_copy(2, NB - 1, 1).wait_recv()

        planned(s, p, LAST)
        step(p, s)
        forward(p, s - 1)

    for s in range(1, 4):
        loop(LAST, functools.partial(level, s))

    def finish(i):
        planned(4, i, PIECES + 1)

        @pl.when(i < LAST)
        def _():
            step(i, 4)
            forward(i, 3)

        @pl.when(i == 1)
        def _():
            wait_all(smalls)
            info[a * NB + b] = own_info()
            start_all(planes(info, isend, irecv))

        @pl.when(i == LAST)
        def _():
            loop(LAST, lambda p: forward(p, 4))
            wait_all(planes(info, isend, irecv))
            info[NA * NB + z] = added(info, 0, NA * NB)
            start_all(lines(info, isend, irecv))

        h = i // PIECES
        multiply(lax.rem(i + h * LAST, PIECES), h)

    loop(2 * PIECES, finish)
    wait_all(lines(info, isend, irecv))
    info[0] = added(info, NA * NB, NZ)

    index = ((x * 2 + c) * NZ + z) * NB + y
    other = ((x * 2 + 1 - c) * NZ + z) * NB + y
    entries = lax.broadcasted_iota(jnp.int32, (voc, 128), 0)
    numbers = [(entries + i * voc).astype(F32) for i in (index, other)]
    left = lane[0:1, :] < 64
    every = info[0]

    def over(line):
        return pltpu.roll(jnp.broadcast_to(line, (8, 128)), 64, 1)[0:1, :]

    for k in range(4):
        ends = [pl.ds(z_at(dist(2 * k + m)), 1) for m in range(2)]
        logits = [acc[k // 2, w, :, (k % 2) * 128 : (k % 2 + 1) * 128] for w in range(2)]
        wanted = jnp.where(left, info[0, ends[0], :], over(info[0, ends[1], :]))
        tops = [jnp.max(part, axis=0, keepdims=True) for part in logits]
        top = jnp.maximum(*tops)
        total = sum(jnp.sum(jnp.exp(part - top), axis=0, keepdims=True) for part in logits)
        picked = sum(
            jnp.sum(jnp.where(number == wanted, part, 0.0), axis=0, keepdims=True)
            for number, part in zip(numbers, logits)
        )
        lse = top + jnp.log(total)
        nllbuf[ends[0], :] = jnp.where(left, lse, over(picked))
        nllbuf[ends[1], :] = jnp.where(left, over(lse), picked)

    def merged(buf, at, n):
        parts = [buf[at + k] for k in range(n)]
        top = functools.reduce(jnp.maximum, parts)
        total = functools.reduce(jnp.add, [jnp.exp(part - top) for part in parts])
        picked = functools.reduce(jnp.add, parts)
        return jnp.where(lane < 64, top + jnp.log(total), picked)

    stat[a * NB + b] = nllbuf[...]
    start_all(planes(stat, ssend, srecv))
    wait_all(planes(stat, ssend, srecv))
    stat[NA * NB + z] = merged(stat, 0, NA * NB)
    start_all(lines(stat, ssend, srecv))
    wait_all(lines(stat, ssend, srecv))
    both = merged(stat, NA * NB, NZ)
    nll = both - pltpu.roll(both, 64, 1)

    codes = jnp.where(lane < 64, pltpu.roll(every, 64, 1), float(NBENCH))
    last_t, last_c = jnp.zeros((8, 128), F32), jnp.zeros((8, 128), F32)
    for j in range(NBENCH):
        hit = codes == float(j)
        part_t = jnp.sum(jnp.where(hit, nll, 0.0), axis=0, keepdims=True)
        part_c = jnp.sum(jnp.where(hit, 1.0, 0.0), axis=0, keepdims=True)
        last_t = jnp.where(row == j, part_t, last_t)
        last_c = jnp.where(row == j, part_c, last_c)
    last[c, 0:8, :] = last_t
    last[c, 8:16, :] = last_c
    swap = rdma(last.at[c], last.at[c], csend, crecv, partner)
    swap.start()

    nllbuf[...] = nll
    mine = nllbuf[pl.ds(z, 1), :]
    rolled = pltpu.roll(jnp.broadcast_to(mine, (8, 128)), lax.rem(128 - base, 128), 1)

    def left_all(ref, ssem, rsem):
        rdma(ref, ref, ssem, rsem, partner).wait_send()

    left_all(abuf.at[:, 0:3], asend, arecv.at[0, 0])
    rdma(weights, wbuf.at[1], wsend, wrecv.at[0], partner).wait_send()
    left_all(gath.at[0:LAST, 0:7, 0], zsend, zrecv.at[0, 0])
    left_all(gath.at[0:LAST, 0:4], bsend, brecv.at[0, 0, 0])
    left_all(gath.at[0:LAST, 0:2], fsend, frecv.at[0, 0])
    left_all(gath.at[LAST, 0, 0:3], ebsend, ebrecv.at[0])
    left_all(gath.at[LAST, 0:7], ezsend, ezrecv.at[0, 0])

    swap.wait()
    sums = jnp.sum(last[0] + last[1], axis=1, keepdims=True)
    row16 = lax.broadcasted_iota(jnp.int32, (16, 128), 0)
    lane16 = lax.broadcasted_iota(jnp.int32, (16, 128), 1)
    sums = jnp.sum(jnp.where(lane16 == row16 + 4, sums, 0.0), axis=0, keepdims=True)
    out[...] = jnp.where(lane[0:1, :] < 4, rolled[0:1, :], sums)


def body(hidden, lm_head, targets, segment, pad_mask, seq_bench):
    tok, width = hidden.shape
    voc = lm_head.shape[1]
    kp = width // PIECES
    tokens = GROUP * tok
    dma = pltpu.SemaphoreType.DMA
    anywhere = pl.BlockSpec(memory_space=pl.ANY)
    vmem = pl.BlockSpec(memory_space=pltpu.VMEM)
    out = pl.pallas_call(
        kernel,
        out_shape=jax.ShapeDtypeStruct((1, 128), F32),
        in_specs=[anywhere] * 6,
        out_specs=vmem,
        scratch_shapes=[
            pltpu.SMEM((tok,), jnp.int32),
            pltpu.SMEM((tok,), jnp.int32),
            pltpu.SMEM((tok,), jnp.int32),
            pltpu.SMEM(seq_bench.shape, jnp.int32),
            pltpu.VMEM((PIECES, NA, tok, kp), jnp.bfloat16),
            pltpu.VMEM((NA * tok, kp), F32),
            pltpu.VMEM((PIECES, NZ, NB, NA * tok, kp), jnp.bfloat16),
            pltpu.VMEM((2, voc, width), jnp.bfloat16),
            pltpu.VMEM((2, 2, voc, tokens // 2), F32),
            pltpu.VMEM((NA * NB + NZ, 8, 128), F32),
            pltpu.VMEM((NA * NB + NZ, 8, 128), F32),
            pltpu.VMEM((2, 16, 128), F32),
            pltpu.VMEM((8, 128), F32),
            dma((4,)), dma((PIECES,)), dma((PIECES,)), dma, dma((PIECES,)),
            dma, dma((PIECES, NA - 1)), dma, dma((LAST, NZ - 1)),
            dma, dma((LAST, 2, NZ)), dma, dma((LAST, NZ)),
            dma, dma((3,)), dma, dma((NB, NZ - 1)),
            dma((NA * NB + NZ,)), dma((NA * NB + NZ,)),
            dma((NA * NB + NZ,)), dma((NA * NB + NZ,)),
            dma, dma,
        ],
        compiler_params=pltpu.CompilerParams(
            collective_id=0, has_side_effects=True, vmem_limit_bytes=62 * 1024 * 1024
        ),
        name="nll",
    )(hidden, lm_head.T, targets, segment, pad_mask, seq_bench)
    line = out[0]
    return (line[:tok], line[tok : tok + NBENCH], line[tok + NBENCH : tok + 2 * NBENCH])


def solution(mesh):
    split = Mesh(mesh.devices.reshape(4, 2, 8, 4), AXES)
    return jax.shard_map(
        body,
        mesh=split,
        in_specs=(P(AXES, None), P(None, AXES), P(AXES), P(AXES), P(AXES), P()),
        out_specs=(P(AXES), P(), P()),
        check_vma=False,
    )
```

```python
import functools

import jax
import jax.numpy as jnp
from jax import lax
from jax.experimental import pallas as pl
from jax.experimental.pallas import tpu as pltpu
from jax.sharding import Mesh
from jax.sharding import PartitionSpec as P

NBENCH = 8
AXES = ("dp_0", "dp_1", "vocab_0", "vocab_1")
NA, NB, NZ = 4, 4, 8
PIECES = 3
WIDE = 2304
LAST = PIECES
GROUP = NA * NB * NZ
PLAN = (
    (
        ("lv", 0, 1), ("ef", 0, 0), ("fw", 0, 0), ("fw", 1, 0), ("lv", 1, 1), ("fw", 2, 0),
        ("lv", 2, 1), ("lv", 0, 2), ("fw", 0, 1), ("lv", 1, 2), ("fw", 1, 1), ("lv", 2, 2),
        ("ez", 0, 0), ("ez", 1, 0), ("ef", 0, 1), ("ez", 2, 0), ("ez", 3, 0), ("fw", 2, 1),
        ("lv", 0, 3), ("fw", 0, 2), ("lv", 1, 3), ("fw", 1, 2), ("lv", 2, 3), ("ez", 0, 1),
        ("fw", 2, 2), ("ez", 1, 1), ("lv", 0, 4), ("ez", 2, 1),
    ),
    (("ez", 3, 1), ("fw", 0, 3), ("lv", 1, 4)),
    (("ez", 0, 2), ("fw", 1, 3), ("lv", 2, 4)),
    (
        ("ez", 1, 2), ("fw", 2, 3), ("fw", 0, 4), ("fw", 1, 4), ("ez", 2, 2), ("fw", 2, 4),
        ("ez", 3, 2), ("ez", 0, 3),
    ),
    (("ez", 1, 3),),
    (("ez", 2, 3), ("ez", 3, 3)),
    (("ez", 0, 4), ("ez", 1, 4)),
    (("ez", 2, 4), ("ez", 3, 4)),
)
MESH = pl.DeviceIdType.MESH
F32 = jnp.float32


def kernel(
    hidden, weights, targets, segment, pad_mask, seq_bench,
    out,
    tgt_s, seg_s, pad_s, ben_s,
    abuf, ebuf, rows32, gath, egath, wbuf, acc, info, stat, last, nllbuf,
    small, lsem, wlsem, wsend, wrecv, asend, easend, arecv, zsend, zrecv,
    bsend, brecv, fsend, frecv, ebsend, ebrecv, ezsend, ezrecv,
    isend, irecv, ssend, srecv, csend, crecv,
):
    x, c = lax.axis_index("dp_0"), lax.axis_index("dp_1")
    z, y = lax.axis_index("vocab_0"), lax.axis_index("vocab_1")
    a = y * (1 - c) + x * c
    b = x * (1 - c) + y * c
    width = weights.shape[1]
    voc = weights.shape[0]

    def dev(a_, b_, z_):
        return (b_ * (1 - c) + a_ * c, c, z_, a_ * (1 - c) + b_ * c)

    def rdma(src, dst, ssem, rsem, to):
        return pltpu.make_async_remote_copy(
            src_ref=src, dst_ref=dst, send_sem=ssem, recv_sem=rsem,
            device_id=to, device_id_type=MESH,
        )

    def a_at(k):
        return lax.rem(a + k, NA)

    def b_at(k):
        return lax.rem(b + k, NB)

    def z_at(k):
        return lax.rem(z + k, NZ)

    partner = (x, 1 - c, z, y)

    def columns(p):
        return slice(p * WIDE, (p + 1) * WIDE if p < LAST else width)

    def held(p):
        return abuf.at[p] if p < LAST else ebuf

    def own_hidden(p):
        return pltpu.make_async_copy(hidden.at[:, columns(p)], held(p).at[a], lsem.at[p])

    def own_weights(p):
        cols = columns(p)
        return pltpu.make_async_copy(weights.at[:, cols], wbuf.at[0, :, cols], wlsem.at[p])

    def swap_weights(p):
        cols = columns(p)
        return rdma(weights.at[:, cols], wbuf.at[1, :, cols], wsend, wrecv.at[p], partner)

    def loop(n, fn):
        lax.fori_loop(0, n, lambda i, _: (fn(i), 0)[1], 0)

    turns = (LAST, *range(PIECES))
    for p in turns:
        own_hidden(p).start()
    smalls = [
        pltpu.make_async_copy(src, dst, small.at[k])
        for k, (src, dst) in enumerate(
            ((targets, tgt_s), (segment, seg_s), (pad_mask, pad_s), (seq_bench, ben_s))
        )
    ]
    for copy in smalls:
        copy.start()

    barrier = pltpu.get_barrier_semaphore()
    peers = [dev(a_at(k), b, z) for k in range(1, NA)]
    peers += [dev(a, b_at(k), z) for k in (1, NB - 1)]
    peers += [dev(a, b, z_at(k)) for k in (1, NZ - 1)]
    peers += [partner]
    for peer in peers:
        pl.semaphore_signal(barrier, inc=1, device_id=peer, device_id_type=MESH)
    pl.semaphore_wait(barrier, len(peers))

    def a_copy(p, k):
        ssem = asend if p < LAST else easend
        mine = held(p).at[a]
        return rdma(mine, mine, ssem, arecv.at[p, k - 1], dev(a_at(k), b, z))

    for p in turns:
        own_hidden(p).wait()
        for k in range(1, NA):
            a_copy(p, k).start()
    for p in range(PIECES + 1):
        own_weights(p).start()
    for p in range(PIECES + 1):
        swap_weights(p).start()
    acc[...] = jnp.zeros(acc.shape, F32)

    def planes(buf, ssem, rsem):
        at = a * NB + b
        return [
            rdma(buf.at[at], buf.at[at], ssem.at[k], rsem.at[k], dev(a_at(k // NB), b_at(k % NB), z))
            for k in range(1, NA * NB)
        ]

    def lines(buf, ssem, rsem):
        at = NA * NB + z
        return [
            rdma(
                buf.at[at], buf.at[at], ssem.at[NA * NB + k], rsem.at[NA * NB + k],
                dev(a, b, z_at(k)),
            )
            for k in range(1, NZ)
        ]

    def start_all(copies):
        for copy in copies:
            copy.start()

    def wait_all(copies):
        for copy in copies:
            copy.wait()

    def added(buf, at, n):
        total = buf[at]
        for k in range(1, n):
            total = total + buf[at + k]
        return total

    def dist(j, odd=None):
        odd = j % 2 if odd is None else odd
        return NZ - 1 - j // 2 if odd else j // 2

    def block(p, b_, z_):
        return egath.at[z_, b_] if p is LAST else gath.at[p, z_, b_]

    def z_copy(p, b_, k, ssem, rsem, up):
        mine = block(p, b_, z_at(k))
        return rdma(mine, mine, ssem, rsem, dev(a, b, z_at(up)))

    def b_send(p, zi, b_, ssem, rsem, go):
        mine = block(p, b_, zi)
        return rdma(mine, mine, ssem, rsem, dev(a, b_at(go), z))

    def b_copy(p, j, way, odd=None):
        go = 1 if way == 0 else NB - 1
        return b_send(p, z_at(dist(j, odd)), b, bsend, brecv.at[p, way, j], go)

    def f_copy(p, j, odd=None):
        odd = j % 2 if odd is None else odd
        come, go = (1, NB - 1) if odd else (NB - 1, 1)
        return b_send(p, z_at(dist(j, odd)), b_at(come), fsend, frecv.at[p, j], go)

    def b_both(p, j):
        b_copy(p, j, 0).start()
        b_copy(p, j, 1).start()

    def e_copy(k, src, go):
        return b_send(LAST, z, b_at(src), ebsend, ebrecv.at[k], go)

    def tile_rows(p):
        wide = held(p).shape[2]
        for k in range(1, NA):
            a_copy(p, k).wait_recv()
        for k in range(NA):
            rows32[4 * k : 4 * k + 4, 0:wide] = held(p)[k].astype(F32)
        tile = rows32[:, 0:wide].astype(jnp.bfloat16)
        if p < LAST:
            gath[p, z, b] = tile
        else:
            egath[z, b] = tile

    def z_step(p, s, u, b_, ssem, rsem):
        odd = u % 2
        if s == 0:
            z_copy(p, b_, 0, ssem, rsem.at[u, 0], 1).start()
            z_copy(p, b_, 0, ssem, rsem.at[u, 1], NZ - 1).start()
        elif s < 4:
            z_copy(p, b_, NZ - s, ssem, rsem.at[u, 2 * s - 2], 1).wait_recv()
            if s < 3:
                z_copy(p, b_, NZ - s, ssem, rsem.at[u, 2 * s], 1).start()
            elif not odd:
                z_copy(p, b_, 5, ssem, rsem.at[u, 6], 1).start()
            z_copy(p, b_, s, ssem, rsem.at[u, 2 * s - 1], NZ - 1).wait_recv()
            if s < 3:
                z_copy(p, b_, s, ssem, rsem.at[u, 2 * s + 1], NZ - 1).start()
            elif odd:
                z_copy(p, b_, 3, ssem, rsem.at[u, 6], NZ - 1).start()
        else:
            z_copy(p, b_, 4, ssem, rsem.at[u, 6], 1).wait_recv()

    def step(p, s):
        z_step(p, s, p, b, zsend, zrecv)
        if s == 0:
            b_both(p, 0)
        elif s < 4:
            b_both(p, 2 * s - 1)
            b_both(p, 2 * s)
        else:
            b_both(p, 7)

    def e_step(u, s):
        z_step(LAST, s, u, b_at((0, 1, 3, 2)[u]), ezsend, ezrecv)

    def e_along(_, s):
        if s == 0:
            e_copy(0, 0, 1).wait_recv()
            e_copy(1, 0, NB - 1).wait_recv()
            e_copy(2, NB - 1, 1).start()
        else:
            e_copy(2, NB - 1, 1).wait_recv()

    def forward(p, s):
        for j in ((0,), (1, 2), (3, 4), (5, 6), (7,))[s]:
            b_copy(p, j, j % 2).wait_recv()
            f_copy(p, j).start()

    def product(h, cols, wide, some):
        rows = jnp.concatenate(
            [some(z_at(dist(4 * h + k, k % 2))).reshape(NB * 16, wide) for k in range(4)], axis=0
        )
        for w in range(2):
            acc[h, w] += lax.dot_general(
                wbuf[w, :, cols], rows, (((1,), (1,)), ((), ())), preferred_element_type=F32
            )

    def multiply(p, h):
        for k in range(4):
            b_copy(p, 4 * h + k, 1 - k % 2, k % 2).wait_recv()
            f_copy(p, 4 * h + k, k % 2).wait_recv()
        cols = pl.ds(pl.multiple_of(p * WIDE, WIDE), WIDE)
        product(h, cols, WIDE, lambda zi: gath[p, zi])

    def multiply_last(h):
        product(h, columns(LAST), width - PIECES * WIDE, lambda zi: egath[zi])

    tile_rows(LAST)
    e_copy(0, 0, 1).start()
    e_copy(1, 0, NB - 1).start()
    for p in range(PIECES):
        tile_rows(p)
        step(p, 0)

    row = lax.broadcasted_iota(jnp.int32, (8, 128), 0)
    lane = lax.broadcasted_iota(jnp.int32, (8, 128), 1)
    base = b * 16 + a * 4

    def own_info():
        own = jnp.zeros((8, 128), jnp.int32)
        whole_last = (x == NA - 1) & (c == 1) & (z == NZ - 1) & (y == NB - 1)
        for t in range(4):
            seg = seg_s[t]
            if t < 3:
                kept = (pad_s[t] == 1) & (seg == seg_s[t + 1])
            else:
                kept = (pad_s[t] == 1) & jnp.logical_not(whole_last)
            code = jnp.where(kept, ben_s[seg], NBENCH)
            own = jnp.where((row == z) & (lane == base + t), tgt_s[t], own)
            own = jnp.where((row == z) & (lane == base + t + 64), code, own)
        return own.astype(F32)

    handle = {"lv": step, "fw": forward, "ez": e_step, "ef": e_along}

    def slot(i):
        for k, things in enumerate(PLAN):

            @pl.when(i == k)
            def _():
                for what, which, s in things:
                    handle[what](which, s)
                if k < PIECES + 1:
                    own_weights(k).wait()
                    swap_weights(k).wait_recv()
                if k == 1:
                    wait_all(smalls)
                    info[a * NB + b] = own_info()
                    start_all(planes(info, isend, irecv))
                if k == 5:
                    wait_all(planes(info, isend, irecv))
                    info[NA * NB + z] = added(info, 0, NA * NB)
                    start_all(lines(info, isend, irecv))

        p, h = lax.rem(i, PIECES + 1), i // (PIECES + 1)

        @pl.when(p < LAST)
        def _():
            multiply(p, h)

        @pl.when(p == LAST)
        def _():
            multiply_last(h)

    loop(len(PLAN), slot)
    wait_all(lines(info, isend, irecv))
    info[0] = added(info, NA * NB, NZ)

    index = ((x * 2 + c) * NZ + z) * NB + y
    other = ((x * 2 + 1 - c) * NZ + z) * NB + y
    entries = lax.broadcasted_iota(jnp.int32, (voc, 128), 0)
    numbers = [(entries + i * voc).astype(F32) for i in (index, other)]
    left = lane[0:1, :] < 64
    every = info[0]

    def over(line):
        return pltpu.roll(jnp.broadcast_to(line, (8, 128)), 64, 1)[0:1, :]

    for k in range(4):
        ends = [pl.ds(z_at(dist(2 * k + m)), 1) for m in range(2)]
        logits = [acc[k // 2, w, :, (k % 2) * 128 : (k % 2 + 1) * 128] for w in range(2)]
        wanted = jnp.where(left, info[0, ends[0], :], over(info[0, ends[1], :]))
        tops = [jnp.max(part, axis=0, keepdims=True) for part in logits]
        top = jnp.maximum(*tops)
        total = sum(jnp.sum(jnp.exp(part - top), axis=0, keepdims=True) for part in logits)
        picked = sum(
            jnp.sum(jnp.where(number == wanted, part, 0.0), axis=0, keepdims=True)
            for number, part in zip(numbers, logits)
        )
        lse = top + jnp.log(total)
        nllbuf[ends[0], :] = jnp.where(left, lse, over(picked))
        nllbuf[ends[1], :] = jnp.where(left, over(lse), picked)

    def merged(buf, at, n):
        parts = [buf[at + k] for k in range(n)]
        top = functools.reduce(jnp.maximum, parts)
        total = functools.reduce(jnp.add, [jnp.exp(part - top) for part in parts])
        picked = functools.reduce(jnp.add, parts)
        return jnp.where(lane < 64, top + jnp.log(total), picked)

    stat[a * NB + b] = nllbuf[...]
    start_all(planes(stat, ssend, srecv))
    wait_all(planes(stat, ssend, srecv))
    stat[NA * NB + z] = merged(stat, 0, NA * NB)
    start_all(lines(stat, ssend, srecv))
    wait_all(lines(stat, ssend, srecv))
    both = merged(stat, NA * NB, NZ)
    nll = both - pltpu.roll(both, 64, 1)

    codes = jnp.where(lane < 64, pltpu.roll(every, 64, 1), float(NBENCH))
    last_t, last_c = jnp.zeros((8, 128), F32), jnp.zeros((8, 128), F32)
    for j in range(NBENCH):
        hit = codes == float(j)
        part_t = jnp.sum(jnp.where(hit, nll, 0.0), axis=0, keepdims=True)
        part_c = jnp.sum(jnp.where(hit, 1.0, 0.0), axis=0, keepdims=True)
        last_t = jnp.where(row == j, part_t, last_t)
        last_c = jnp.where(row == j, part_c, last_c)
    last[c, 0:8, :] = last_t
    last[c, 8:16, :] = last_c
    swap = rdma(last.at[c], last.at[c], csend, crecv, partner)
    swap.start()

    nllbuf[...] = nll
    mine = nllbuf[pl.ds(z, 1), :]
    rolled = pltpu.roll(jnp.broadcast_to(mine, (8, 128)), lax.rem(128 - base, 128), 1)

    def left_all(ref, ssem, rsem):
        rdma(ref, ref, ssem, rsem, partner).wait_send()

    left_all(abuf.at[:, 0:3], asend, arecv.at[0, 0])
    left_all(ebuf.at[0:3], easend, arecv.at[0, 0])
    rdma(weights, wbuf.at[1], wsend, wrecv.at[0], partner).wait_send()
    left_all(gath.at[:, 0:7, 0], zsend, zrecv.at[0, 0])
    left_all(gath.at[:, 0:4], bsend, brecv.at[0, 0, 0])
    left_all(gath.at[:, 0:2], fsend, frecv.at[0, 0])
    left_all(egath.at[0, 0:3], ebsend, ebrecv.at[0])
    left_all(egath.at[0:7], ezsend, ezrecv.at[0, 0])

    swap.wait()
    sums = jnp.sum(last[0] + last[1], axis=1, keepdims=True)
    row16 = lax.broadcasted_iota(jnp.int32, (16, 128), 0)
    lane16 = lax.broadcasted_iota(jnp.int32, (16, 128), 1)
    sums = jnp.sum(jnp.where(lane16 == row16 + 4, sums, 0.0), axis=0, keepdims=True)
    out[...] = jnp.where(lane[0:1, :] < 4, rolled[0:1, :], sums)


def body(hidden, lm_head, targets, segment, pad_mask, seq_bench):
    tok, width = hidden.shape
    voc = lm_head.shape[1]
    rest = width - PIECES * WIDE
    tokens = GROUP * tok
    dma = pltpu.SemaphoreType.DMA
    anywhere = pl.BlockSpec(memory_space=pl.ANY)
    vmem = pl.BlockSpec(memory_space=pltpu.VMEM)
    out = pl.pallas_call(
        kernel,
        out_shape=jax.ShapeDtypeStruct((1, 128), F32),
        in_specs=[anywhere] * 6,
        out_specs=vmem,
        scratch_shapes=[
            pltpu.SMEM((tok,), jnp.int32),
            pltpu.SMEM((tok,), jnp.int32),
            pltpu.SMEM((tok,), jnp.int32),
            pltpu.SMEM(seq_bench.shape, jnp.int32),
            pltpu.VMEM((PIECES, NA, tok, WIDE), jnp.bfloat16),
            pltpu.VMEM((NA, tok, rest), jnp.bfloat16),
            pltpu.VMEM((NA * tok, WIDE), F32),
            pltpu.VMEM((PIECES, NZ, NB, NA * tok, WIDE), jnp.bfloat16),
            pltpu.VMEM((NZ, NB, NA * tok, rest), jnp.bfloat16),
            pltpu.VMEM((2, voc, width), jnp.bfloat16),
            pltpu.VMEM((2, 2, voc, tokens // 2), F32),
            pltpu.VMEM((NA * NB + NZ, 8, 128), F32),
            pltpu.VMEM((NA * NB + NZ, 8, 128), F32),
            pltpu.VMEM((2, 16, 128), F32),
            pltpu.VMEM((8, 128), F32),
            dma((4,)), dma((PIECES + 1,)), dma((PIECES + 1,)), dma, dma((PIECES + 1,)),
            dma, dma, dma((PIECES + 1, NA - 1)), dma, dma((PIECES, NZ - 1)),
            dma, dma((PIECES, 2, NZ)), dma, dma((PIECES, NZ)),
            dma, dma((3,)), dma, dma((NB, NZ - 1)),
            dma((NA * NB + NZ,)), dma((NA * NB + NZ,)),
            dma((NA * NB + NZ,)), dma((NA * NB + NZ,)),
            dma, dma,
        ],
        compiler_params=pltpu.CompilerParams(
            collective_id=0, has_side_effects=True, vmem_limit_bytes=62 * 1024 * 1024
        ),
        name="nll",
    )(hidden, lm_head.T, targets, segment, pad_mask, seq_bench)

    def split(line, first, second, third):
        first[...] = line[:, 0:tok]
        second[...] = line[:, tok : tok + NBENCH]
        third[...] = line[:, tok + NBENCH : tok + 2 * NBENCH]

    nll, total, count = pl.pallas_call(
        split,
        out_shape=(
            jax.ShapeDtypeStruct((1, tok), F32),
            jax.ShapeDtypeStruct((1, NBENCH), F32),
            jax.ShapeDtypeStruct((1, NBENCH), F32),
        ),
        name="split",
    )(out)
    return (nll.reshape(tok), total.reshape(NBENCH), count.reshape(NBENCH))


def solution(mesh):
    split = Mesh(mesh.devices.reshape(4, 2, 8, 4), AXES)
    return jax.shard_map(
        body,
        mesh=split,
        in_specs=(P(AXES, None), P(None, AXES), P(AXES), P(AXES), P(AXES), P()),
        out_specs=(P(AXES), P(), P()),
        check_vma=False,
    )
```

```python
import functools

import jax
import jax.numpy as jnp
from jax import lax
from jax.experimental import pallas as pl
from jax.experimental.pallas import tpu as pltpu
from jax.sharding import Mesh
from jax.sharding import PartitionSpec as P

NBENCH = 8
AXES = ("dp_0", "dp_1", "vocab_0", "vocab_1")
NA, NB, NZ = 4, 4, 8
PIECES = 3
WIDE = 2304
LAST = PIECES
GROUP = NA * NB * NZ
PLAN = (
    (
        ("lv", 0, 1), ("ef", 0, 0), ("fw", 0, 0), ("fw", 1, 0), ("lv", 1, 1), ("fw", 2, 0),
        ("lv", 2, 1), ("lv", 0, 2), ("fw", 0, 1), ("lv", 1, 2), ("fw", 1, 1), ("lv", 2, 2),
        ("ez", 0, 0), ("ez", 1, 0), ("ef", 0, 1), ("in", 0, 0), ("ez", 2, 0), ("ez", 3, 0), ("fw", 2, 1),
        ("lv", 0, 3), ("fw", 0, 2), ("lv", 1, 3), ("fw", 1, 2), ("lv", 2, 3), ("ez", 0, 1),
        ("fw", 2, 2), ("ez", 1, 1), ("lv", 0, 4), ("in", 0, 1),
        ("ez", 2, 1),
    ),
    (("ez", 3, 1), ("fw", 0, 3), ("lv", 1, 4)),
    (("ez", 0, 2), ("fw", 1, 3), ("lv", 2, 4)),
    (
        ("ez", 1, 2), ("fw", 2, 3), ("fw", 0, 4), ("fw", 1, 4), ("ez", 2, 2), ("fw", 2, 4),
        ("ez", 3, 2), ("ez", 0, 3),
    ),
    (("in", 0, 2), ("ez", 1, 3)),
    (("ez", 2, 3), ("ez", 3, 3)),
    (("ez", 0, 4), ("ez", 1, 4)),
    (("ez", 2, 4), ("ez", 3, 4)),
)
MESH = pl.DeviceIdType.MESH
F32 = jnp.float32


def kernel(
    hidden, weights, targets, segment, pad_mask, seq_bench,
    out,
    tgt_s, seg_s, pad_s, ben_s,
    abuf, ebuf, rows32, gath, egath, wbuf, acc, info, stat, xinfo, xstat, nllbuf,
    small, lsem, wlsem, wsend, wrecv, asend, easend, arecv, zsend, zrecv,
    bsend, brecv, fsend, frecv, ebsend, ebrecv, ezsend, ezrecv,
    isend, irecv, ssend, srecv, xisend, xirecv, xssend, xsrecv,
):
    x, c = lax.axis_index("dp_0"), lax.axis_index("dp_1")
    z, y = lax.axis_index("vocab_0"), lax.axis_index("vocab_1")
    a = y * (1 - c) + x * c
    b = x * (1 - c) + y * c
    width = weights.shape[1]
    voc = weights.shape[0]

    def dev(a_, b_, z_):
        return (b_ * (1 - c) + a_ * c, c, z_, a_ * (1 - c) + b_ * c)

    def rdma(src, dst, ssem, rsem, to):
        return pltpu.make_async_remote_copy(
            src_ref=src, dst_ref=dst, send_sem=ssem, recv_sem=rsem,
            device_id=to, device_id_type=MESH,
        )

    def a_at(k):
        return lax.rem(a + k, NA)

    def b_at(k):
        return lax.rem(b + k, NB)

    def z_at(k):
        return lax.rem(z + k, NZ)

    partner = (x, 1 - c, z, y)

    def columns(p):
        return slice(p * WIDE, (p + 1) * WIDE if p < LAST else width)

    def held(p):
        return abuf.at[p] if p < LAST else ebuf

    def own_hidden(p):
        return pltpu.make_async_copy(hidden.at[:, columns(p)], held(p).at[a], lsem.at[p])

    def own_weights(p):
        cols = columns(p)
        return pltpu.make_async_copy(weights.at[:, cols], wbuf.at[0, :, cols], wlsem.at[p])

    def swap_weights(p):
        cols = columns(p)
        return rdma(weights.at[:, cols], wbuf.at[1, :, cols], wsend, wrecv.at[p], partner)

    def loop(n, fn):
        lax.fori_loop(0, n, lambda i, _: (fn(i), 0)[1], 0)

    turns = (LAST, *range(PIECES))
    for p in turns:
        own_hidden(p).start()
    smalls = [
        pltpu.make_async_copy(src, dst, small.at[k])
        for k, (src, dst) in enumerate(
            ((targets, tgt_s), (segment, seg_s), (pad_mask, pad_s), (seq_bench, ben_s))
        )
    ]
    for copy in smalls:
        copy.start()

    barrier = pltpu.get_barrier_semaphore()
    peers = [dev(a_at(k), b, z) for k in range(1, NA)]
    peers += [dev(a, b_at(k), z) for k in (1, NB - 1)]
    peers += [dev(a, b, z_at(k)) for k in (1, NZ - 1)]
    peers += [partner]
    for peer in peers:
        pl.semaphore_signal(barrier, inc=1, device_id=peer, device_id_type=MESH)
    pl.semaphore_wait(barrier, len(peers))

    def a_copy(p, k):
        ssem = asend if p < LAST else easend
        mine = held(p).at[a]
        return rdma(mine, mine, ssem, arecv.at[p, k - 1], dev(a_at(k), b, z))

    for p in turns:
        own_hidden(p).wait()
        for k in range(1, NA):
            a_copy(p, k).start()
    for p in range(PIECES + 1):
        own_weights(p).start()
    for p in range(PIECES + 1):
        swap_weights(p).start()
    acc[...] = jnp.zeros(acc.shape, F32)

    def planes(buf, ssem, rsem):
        at = a * NB + b
        return [
            rdma(buf.at[at], buf.at[at], ssem.at[k], rsem.at[k], dev(a_at(k // NB), b_at(k % NB), z))
            for k in range(1, NA * NB)
        ]

    def lines(buf, ssem, rsem):
        at = NA * NB + z
        return [
            rdma(
                buf.at[at], buf.at[at], ssem.at[NA * NB + k], rsem.at[NA * NB + k],
                dev(a, b, z_at(k)),
            )
            for k in range(1, NZ)
        ]

    def crossings(buf, far, ssem, rsem):
        return [
            rdma(
                buf.at[NA * NB + z], far.at[z], ssem.at[k], rsem.at[k], (x, 1 - c, z_at(k), y)
            )
            for k in range(NZ)
        ]

    def start_all(copies):
        for copy in copies:
            copy.start()

    def wait_all(copies):
        for copy in copies:
            copy.wait()

    def added(buf, at, n):
        total = buf[at]
        for k in range(1, n):
            total = total + buf[at + k]
        return total

    def dist(j, odd=None):
        odd = j % 2 if odd is None else odd
        return NZ - 1 - j // 2 if odd else j // 2

    def block(p, b_, z_):
        return egath.at[z_, b_] if p is LAST else gath.at[p, z_, b_]

    def z_copy(p, b_, k, ssem, rsem, up):
        mine = block(p, b_, z_at(k))
        return rdma(mine, mine, ssem, rsem, dev(a, b, z_at(up)))

    def b_send(p, zi, b_, ssem, rsem, go):
        mine = block(p, b_, zi)
        return rdma(mine, mine, ssem, rsem, dev(a, b_at(go), z))

    def b_copy(p, j, way, odd=None):
        go = 1 if way == 0 else NB - 1
        return b_send(p, z_at(dist(j, odd)), b, bsend, brecv.at[p, way, j], go)

    def f_copy(p, j, odd=None):
        odd = j % 2 if odd is None else odd
        come, go = (1, NB - 1) if odd else (NB - 1, 1)
        return b_send(p, z_at(dist(j, odd)), b_at(come), fsend, frecv.at[p, j], go)

    def b_both(p, j):
        b_copy(p, j, 0).start()
        b_copy(p, j, 1).start()

    def e_copy(k, src, go):
        return b_send(LAST, z, b_at(src), ebsend, ebrecv.at[k], go)

    def tile_rows(p):
        wide = held(p).shape[2]
        for k in range(1, NA):
            a_copy(p, k).wait_recv()
        for k in range(NA):
            rows32[4 * k : 4 * k + 4, 0:wide] = held(p)[k].astype(F32)
        tile = rows32[:, 0:wide].astype(jnp.bfloat16)
        if p < LAST:
            gath[p, z, b] = tile
        else:
            egath[z, b] = tile

    def z_step(p, s, u, b_, ssem, rsem):
        odd = u % 2
        if s == 0:
            z_copy(p, b_, 0, ssem, rsem.at[u, 0], 1).start()
            z_copy(p, b_, 0, ssem, rsem.at[u, 1], NZ - 1).start()
        elif s < 4:
            z_copy(p, b_, NZ - s, ssem, rsem.at[u, 2 * s - 2], 1).wait_recv()
            if s < 3:
                z_copy(p, b_, NZ - s, ssem, rsem.at[u, 2 * s], 1).start()
            elif not odd:
                z_copy(p, b_, 5, ssem, rsem.at[u, 6], 1).start()
            z_copy(p, b_, s, ssem, rsem.at[u, 2 * s - 1], NZ - 1).wait_recv()
            if s < 3:
                z_copy(p, b_, s, ssem, rsem.at[u, 2 * s + 1], NZ - 1).start()
            elif odd:
                z_copy(p, b_, 3, ssem, rsem.at[u, 6], NZ - 1).start()
        else:
            z_copy(p, b_, 4, ssem, rsem.at[u, 6], 1).wait_recv()

    def step(p, s):
        z_step(p, s, p, b, zsend, zrecv)
        if s == 0:
            b_both(p, 0)
        elif s < 4:
            b_both(p, 2 * s - 1)
            b_both(p, 2 * s)
        else:
            b_both(p, 7)

    def e_step(u, s):
        z_step(LAST, s, u, b_at((0, 1, 3, 2)[u]), ezsend, ezrecv)

    def e_along(_, s):
        if s == 0:
            e_copy(0, 0, 1).wait_recv()
            e_copy(1, 0, NB - 1).wait_recv()
            e_copy(2, NB - 1, 1).start()
        else:
            e_copy(2, NB - 1, 1).wait_recv()

    def forward(p, s):
        for j in ((0,), (1, 2), (3, 4), (5, 6), (7,))[s]:
            b_copy(p, j, j % 2).wait_recv()
            f_copy(p, j).start()

    def product(h, cols, wide, some):
        rows = jnp.concatenate(
            [some(z_at(dist(4 * h + k, k % 2))).reshape(NB * 16, wide) for k in range(4)], axis=0
        )
        for w in range(2):
            acc[h, w] += lax.dot_general(
                wbuf[w, :, cols], rows, (((1,), (1,)), ((), ())), preferred_element_type=F32
            )

    def multiply(p, h):
        for k in range(4):
            b_copy(p, 4 * h + k, 1 - k % 2, k % 2).wait_recv()
            f_copy(p, 4 * h + k, k % 2).wait_recv()
        cols = pl.ds(pl.multiple_of(p * WIDE, WIDE), WIDE)
        product(h, cols, WIDE, lambda zi: gath[p, zi])

    def multiply_last(h):
        product(h, columns(LAST), width - PIECES * WIDE, lambda zi: egath[zi])

    tile_rows(LAST)
    e_copy(0, 0, 1).start()
    e_copy(1, 0, NB - 1).start()
    for p in range(PIECES):
        tile_rows(p)
        step(p, 0)

    row = lax.broadcasted_iota(jnp.int32, (8, 128), 0)
    lane = lax.broadcasted_iota(jnp.int32, (8, 128), 1)
    base = b * 16 + a * 4

    def own_info():
        own = jnp.zeros((8, 128), jnp.int32)
        whole_last = (x == NA - 1) & (c == 1) & (z == NZ - 1) & (y == NB - 1)
        for t in range(4):
            seg = seg_s[t]
            if t < 3:
                kept = (pad_s[t] == 1) & (seg == seg_s[t + 1])
            else:
                kept = (pad_s[t] == 1) & jnp.logical_not(whole_last)
            code = jnp.where(kept, ben_s[seg], NBENCH)
            own = jnp.where(lane == base + t, tgt_s[t], own)
            own = jnp.where(lane == base + t + 64, code, own)
        return own.astype(F32)

    def along_info(_, s):
        if s == 0:
            wait_all(smalls)
            info[a * NB + b] = own_info()[0:1]
            start_all(planes(info, isend, irecv))
        elif s == 1:
            wait_all(planes(info, isend, irecv))
            info[NA * NB + z] = added(info, 0, NA * NB)
            start_all(lines(info, isend, irecv))
            start_all(crossings(info, xinfo, xisend, xirecv))
        else:
            wait_all(lines(info, isend, irecv))
            wait_all(crossings(info, xinfo, xisend, xirecv))

    index = ((x * 2 + c) * NZ + z) * NB + y
    other = ((x * 2 + 1 - c) * NZ + z) * NB + y
    entries = lax.broadcasted_iota(jnp.int32, (voc, 128), 0)
    numbers = [(entries + i * voc).astype(F32) for i in (index, other)]
    left = lane[0:1, :] < 64

    def over(line):
        return pltpu.roll(jnp.broadcast_to(line, (8, 128)), 64, 1)[0:1, :]

    def statistics(h):
        for k in (2 * h, 2 * h + 1):
            near = [z_at(dist(2 * k + m)) for m in range(2)]
            ends = [pl.ds(zi, 1) for zi in near]
            logits = [acc[k // 2, w, :, (k % 2) * 128 : (k % 2 + 1) * 128] for w in range(2)]
            wanted = jnp.where(left, info[NA * NB + near[0]], over(info[NA * NB + near[1]]))
            tops = [jnp.max(part, axis=0, keepdims=True) for part in logits]
            top = jnp.maximum(*tops)
            total = sum(jnp.sum(jnp.exp(part - top), axis=0, keepdims=True) for part in logits)
            picked = sum(
                jnp.sum(jnp.where(number == wanted, part, 0.0), axis=0, keepdims=True)
                for number, part in zip(numbers, logits)
            )
            lse = top + jnp.log(total)
            nllbuf[ends[0], :] = jnp.where(left, lse, over(picked))
            nllbuf[ends[1], :] = jnp.where(left, over(lse), picked)

    handle = {"lv": step, "fw": forward, "ez": e_step, "ef": e_along, "in": along_info}

    def slot(i):
        for k, things in enumerate(PLAN):

            @pl.when(i == k)
            def _():
                for what, which, s in things:
                    handle[what](which, s)
                if k < PIECES + 1:
                    own_weights(k).wait()
                    swap_weights(k).wait_recv()
                if k == 6:
                    statistics(0)

        p, h = lax.rem(i, PIECES + 1), i // (PIECES + 1)

        @pl.when(p < LAST)
        def _():
            multiply(p, h)

        @pl.when(p == LAST)
        def _():
            multiply_last(h)

    loop(len(PLAN), slot)
    statistics(1)
    def merged(buf, at, n):
        parts = [buf[at + k] for k in range(n)]
        top = functools.reduce(jnp.maximum, parts)
        total = functools.reduce(jnp.add, [jnp.exp(part - top) for part in parts])
        picked = functools.reduce(jnp.add, parts)
        return jnp.where(lane < 64, top + jnp.log(total), picked)

    stat[a * NB + b] = nllbuf[...]
    start_all(planes(stat, ssend, srecv))
    wait_all(planes(stat, ssend, srecv))
    stat[NA * NB + z] = merged(stat, 0, NA * NB)
    start_all(lines(stat, ssend, srecv))
    start_all(crossings(stat, xstat, xssend, xsrecv))
    def left_all(ref, ssem, rsem):
        rdma(ref, ref, ssem, rsem, partner).wait_send()

    left_all(abuf.at[:, 0:3], asend, arecv.at[0, 0])
    left_all(ebuf.at[0:3], easend, arecv.at[0, 0])
    rdma(weights, wbuf.at[1], wsend, wrecv.at[0], partner).wait_send()
    left_all(gath.at[:, 0:7, 0], zsend, zrecv.at[0, 0])
    left_all(gath.at[:, 0:4], bsend, brecv.at[0, 0, 0])
    left_all(gath.at[:, 0:2], fsend, frecv.at[0, 0])
    left_all(egath.at[0, 0:3], ebsend, ebrecv.at[0])
    left_all(egath.at[0:7], ezsend, ezrecv.at[0, 0])

    def losses(buf, at):
        both = merged(buf, at, NZ)
        return both - pltpu.roll(both, 64, 1)

    def gathered(buf, at):
        return jnp.concatenate([buf[at + k] for k in range(NZ)], axis=0)

    def by_core(mine, others, first, second):
        lower, upper = jnp.where(c == 0, mine, others), jnp.where(c == 0, others, mine)
        lower = pltpu.roll(lower, 64, 1) if first else lower
        upper = pltpu.roll(upper, 64, 1) if second else upper
        return jnp.where(lane < 64, lower, upper)

    codes = by_core(gathered(info, NA * NB), gathered(xinfo, 0), True, False)
    wait_all(lines(stat, ssend, srecv))
    nll = losses(stat, NA * NB)
    nllbuf[...] = nll
    mine = nllbuf[pl.ds(z, 1), :]
    rolled = pltpu.roll(jnp.broadcast_to(mine, (8, 128)), lax.rem(128 - base, 128), 1)
    wait_all(crossings(stat, xstat, xssend, xsrecv))
    loss = by_core(nll, losses(xstat, 0), False, True)
    last_t, last_c = jnp.zeros((8, 128), F32), jnp.zeros((8, 128), F32)
    for j in range(NBENCH):
        hit = codes == float(j)
        part_t = jnp.sum(jnp.where(hit, loss, 0.0), axis=0, keepdims=True)
        part_c = jnp.sum(jnp.where(hit, 1.0, 0.0), axis=0, keepdims=True)
        last_t = jnp.where(row == j, part_t, last_t)
        last_c = jnp.where(row == j, part_c, last_c)
    sums = jnp.sum(jnp.concatenate([last_t, last_c], axis=0), axis=1, keepdims=True)
    row16 = lax.broadcasted_iota(jnp.int32, (16, 128), 0)
    lane16 = lax.broadcasted_iota(jnp.int32, (16, 128), 1)
    sums = jnp.sum(jnp.where(lane16 == row16 + 4, sums, 0.0), axis=0, keepdims=True)
    out[...] = jnp.where(lane[0:1, :] < 4, rolled[0:1, :], sums)


def body(hidden, lm_head, targets, segment, pad_mask, seq_bench):
    tok, width = hidden.shape
    voc = lm_head.shape[1]
    rest = width - PIECES * WIDE
    tokens = GROUP * tok
    dma = pltpu.SemaphoreType.DMA
    anywhere = pl.BlockSpec(memory_space=pl.ANY)
    vmem = pl.BlockSpec(memory_space=pltpu.VMEM)
    out = pl.pallas_call(
        kernel,
        out_shape=jax.ShapeDtypeStruct((1, 128), F32),
        in_specs=[anywhere] * 6,
        out_specs=vmem,
        scratch_shapes=[
            pltpu.SMEM((tok,), jnp.int32),
            pltpu.SMEM((tok,), jnp.int32),
            pltpu.SMEM((tok,), jnp.int32),
            pltpu.SMEM(seq_bench.shape, jnp.int32),
            pltpu.VMEM((PIECES, NA, tok, WIDE), jnp.bfloat16),
            pltpu.VMEM((NA, tok, rest), jnp.bfloat16),
            pltpu.VMEM((NA * tok, WIDE), F32),
            pltpu.VMEM((PIECES, NZ, NB, NA * tok, WIDE), jnp.bfloat16),
            pltpu.VMEM((NZ, NB, NA * tok, rest), jnp.bfloat16),
            pltpu.VMEM((2, voc, width), jnp.bfloat16),
            pltpu.VMEM((2, 2, voc, tokens // 2), F32),
            pltpu.VMEM((NA * NB + NZ, 1, 128), F32),
            pltpu.VMEM((NA * NB + NZ, 8, 128), F32),
            pltpu.VMEM((NZ, 1, 128), F32),
            pltpu.VMEM((NZ, 8, 128), F32),
            pltpu.VMEM((8, 128), F32),
            dma((4,)), dma((PIECES + 1,)), dma((PIECES + 1,)), dma, dma((PIECES + 1,)),
            dma, dma, dma((PIECES + 1, NA - 1)), dma, dma((PIECES, NZ - 1)),
            dma, dma((PIECES, 2, NZ)), dma, dma((PIECES, NZ)),
            dma, dma((3,)), dma, dma((NB, NZ - 1)),
            dma((NA * NB + NZ,)), dma((NA * NB + NZ,)),
            dma((NA * NB + NZ,)), dma((NA * NB + NZ,)),
            dma((NZ,)), dma((NZ,)), dma((NZ,)), dma((NZ,)),
        ],
        compiler_params=pltpu.CompilerParams(
            collective_id=0, has_side_effects=True, vmem_limit_bytes=62 * 1024 * 1024
        ),
        name="nll",
    )(hidden, lm_head.T, targets, segment, pad_mask, seq_bench)

    def split(line, first, second, third):
        first[...] = line[:, 0:tok]
        second[...] = line[:, tok : tok + NBENCH]
        third[...] = line[:, tok + NBENCH : tok + 2 * NBENCH]

    nll, total, count = pl.pallas_call(
        split,
        out_shape=(
            jax.ShapeDtypeStruct((1, tok), F32),
            jax.ShapeDtypeStruct((1, NBENCH), F32),
            jax.ShapeDtypeStruct((1, NBENCH), F32),
        ),
        name="split",
    )(out)
    return (nll.reshape(tok), total.reshape(NBENCH), count.reshape(NBENCH))


def solution(mesh):
    split = Mesh(mesh.devices.reshape(4, 2, 8, 4), AXES)
    return jax.shard_map(
        body,
        mesh=split,
        in_specs=(P(AXES, None), P(None, AXES), P(AXES), P(AXES), P(AXES), P()),
        out_specs=(P(AXES), P(), P()),
        check_vma=False,
    )
```

```python
import functools

import jax
import jax.numpy as jnp
from jax import lax
from jax.experimental import pallas as pl
from jax.experimental.pallas import tpu as pltpu
from jax.sharding import Mesh
from jax.sharding import PartitionSpec as P

NBENCH = 8
AXES = ("dp_0", "dp_1", "vocab_0", "vocab_1")
NA, NB, NZ = 4, 4, 8
PIECES = 3
WIDE = 2304
LAST = PIECES
GROUP = NA * NB * NZ
PLAN = (
    (
        ("ef", 0, 0), ("fw", 0, 0), ("lv", 0, 1), ("lv", 1, 1), ("lv", 2, 1), ("lv", 0, 2),
        ("fw", 1, 0), ("lv", 1, 2), ("ef", 0, 1), ("in", 0, 0), ("ez", 3, 0), ("lv", 2, 2),
        ("fw", 2, 1), ("fw", 0, 1), ("fw", 0, 2), ("ez", 2, 0), ("fw", 1, 1), ("lv", 0, 3),
        ("ez", 1, 0), ("ez", 0, 0), ("fw", 2, 0), ("ez", 3, 1), ("fw", 1, 2), ("fw", 2, 2),
        ("ez", 2, 1), ("lv", 1, 3), ("lv", 0, 4), ("in", 0, 1), ("lv", 2, 3),
    ),
    (("ez", 1, 1), ("ez", 0, 1)),
    (("ez", 3, 2), ("fw", 0, 3), ("ez", 2, 2), ("lv", 1, 4)),
    (
        ("lv", 2, 4), ("fw", 0, 4), ("ez", 1, 2), ("fw", 1, 3), ("ez", 0, 2), ("fw", 1, 4),
    ),
    (("fw", 2, 3), ("ez", 2, 3), ("fw", 2, 4), ("ez", 3, 3)),
    (("ez", 1, 3), ("ez", 0, 3), ("in", 0, 2)),
    (("ez", 3, 4), ("ez", 2, 4)),
    (("ez", 1, 4), ("ez", 0, 4)),
)
MESH = pl.DeviceIdType.MESH
F32 = jnp.float32


def kernel(
    hidden, weights, targets, segment, pad_mask, seq_bench,
    out,
    tgt_s, seg_s, pad_s, ben_s,
    abuf, ebuf, rows32, gath, egath, wbuf, acc, info, stat, xinfo, xstat, nllbuf,
    small, lsem, wlsem, wsend, wrecv, asend, easend, arecv, zsend, zrecv,
    bsend, brecv, fsend, frecv, ebsend, ebrecv, ezsend, ezrecv,
    isend, irecv, ssend, srecv, xisend, xirecv, xssend, xsrecv,
):
    x, c = lax.axis_index("dp_0"), lax.axis_index("dp_1")
    z, y = lax.axis_index("vocab_0"), lax.axis_index("vocab_1")
    a = y * (1 - c) + x * c
    b = x * (1 - c) + y * c
    width = weights.shape[1]
    voc = weights.shape[0]

    def dev(a_, b_, z_):
        return (b_ * (1 - c) + a_ * c, c, z_, a_ * (1 - c) + b_ * c)

    def rdma(src, dst, ssem, rsem, to):
        return pltpu.make_async_remote_copy(
            src_ref=src, dst_ref=dst, send_sem=ssem, recv_sem=rsem,
            device_id=to, device_id_type=MESH,
        )

    def a_at(k):
        return lax.rem(a + k, NA)

    def b_at(k):
        return lax.rem(b + k, NB)

    def z_at(k):
        return lax.rem(z + k, NZ)

    partner = (x, 1 - c, z, y)

    def columns(p):
        return slice(p * WIDE, (p + 1) * WIDE if p < LAST else width)

    def held(p):
        return abuf.at[p] if p < LAST else ebuf

    def own_hidden(p):
        return pltpu.make_async_copy(hidden.at[:, columns(p)], held(p).at[a], lsem.at[p])

    def own_weights(p):
        cols = columns(p)
        return pltpu.make_async_copy(weights.at[:, cols], wbuf.at[0, :, cols], wlsem.at[p])

    def swap_weights(p):
        cols = columns(p)
        return rdma(weights.at[:, cols], wbuf.at[1, :, cols], wsend, wrecv.at[p], partner)

    def loop(n, fn):
        lax.fori_loop(0, n, lambda i, _: (fn(i), 0)[1], 0)

    turns = (LAST, *range(PIECES))
    for p in turns:
        own_hidden(p).start()
    smalls = [
        pltpu.make_async_copy(src, dst, small.at[k])
        for k, (src, dst) in enumerate(
            ((targets, tgt_s), (segment, seg_s), (pad_mask, pad_s), (seq_bench, ben_s))
        )
    ]
    for copy in smalls:
        copy.start()

    barrier = pltpu.get_barrier_semaphore()
    peers = [dev(a_at(k), b, z) for k in range(1, NA)]
    peers += [dev(a, b_at(k), z) for k in (1, NB - 1)]
    peers += [dev(a, b, z_at(k)) for k in (1, NZ - 1)]
    peers += [partner]
    for peer in peers:
        pl.semaphore_signal(barrier, inc=1, device_id=peer, device_id_type=MESH)
    pl.semaphore_wait(barrier, len(peers))

    def a_copy(p, k):
        ssem = asend if p < LAST else easend
        mine = held(p).at[a]
        return rdma(mine, mine, ssem, arecv.at[p, k - 1], dev(a_at(k), b, z))

    for p in turns:
        own_hidden(p).wait()
        for k in range(1, NA):
            a_copy(p, k).start()
    for p in range(PIECES + 1):
        own_weights(p).start()
    for p in range(PIECES + 1):
        swap_weights(p).start()
    acc[...] = jnp.zeros(acc.shape, F32)

    def planes(buf, ssem, rsem):
        at = a * NB + b
        return [
            rdma(buf.at[at], buf.at[at], ssem.at[k], rsem.at[k], dev(a_at(k // NB), b_at(k % NB), z))
            for k in range(1, NA * NB)
        ]

    def lines(buf, ssem, rsem):
        at = NA * NB + z
        return [
            rdma(
                buf.at[at], buf.at[at], ssem.at[NA * NB + k], rsem.at[NA * NB + k],
                dev(a, b, z_at(k)),
            )
            for k in range(1, NZ)
        ]

    def crossings(buf, far, ssem, rsem):
        return [
            rdma(
                buf.at[NA * NB + z], far.at[z], ssem.at[k], rsem.at[k], (x, 1 - c, z_at(k), y)
            )
            for k in range(NZ)
        ]

    def start_all(copies):
        for copy in copies:
            copy.start()

    def wait_all(copies):
        for copy in copies:
            copy.wait()

    def added(buf, at, n):
        total = buf[at]
        for k in range(1, n):
            total = total + buf[at + k]
        return total

    def dist(j, odd=None):
        odd = j % 2 if odd is None else odd
        return NZ - 1 - j // 2 if odd else j // 2

    def block(p, b_, z_):
        return egath.at[z_, b_] if p is LAST else gath.at[p, z_, b_]

    def z_copy(p, b_, k, ssem, rsem, up):
        mine = block(p, b_, z_at(k))
        return rdma(mine, mine, ssem, rsem, dev(a, b, z_at(up)))

    def b_send(p, zi, b_, ssem, rsem, go):
        mine = block(p, b_, zi)
        return rdma(mine, mine, ssem, rsem, dev(a, b_at(go), z))

    def b_copy(p, j, way, odd=None):
        go = 1 if way == 0 else NB - 1
        return b_send(p, z_at(dist(j, odd)), b, bsend, brecv.at[p, way, j], go)

    def f_copy(p, j, odd=None):
        odd = j % 2 if odd is None else odd
        come, go = (1, NB - 1) if odd else (NB - 1, 1)
        return b_send(p, z_at(dist(j, odd)), b_at(come), fsend, frecv.at[p, j], go)

    def b_both(p, j):
        b_copy(p, j, 0).start()
        b_copy(p, j, 1).start()

    def e_copy(k, src, go):
        return b_send(LAST, z, b_at(src), ebsend, ebrecv.at[k], go)

    def tile_rows(p):
        wide = held(p).shape[2]
        for k in range(1, NA):
            a_copy(p, k).wait_recv()
        for k in range(NA):
            rows32[4 * k : 4 * k + 4, 0:wide] = held(p)[k].astype(F32)
        tile = rows32[:, 0:wide].astype(jnp.bfloat16)
        if p < LAST:
            gath[p, z, b] = tile
        else:
            egath[z, b] = tile

    def z_step(p, s, u, b_, ssem, rsem):
        odd = u % 2
        if s == 0:
            z_copy(p, b_, 0, ssem, rsem.at[u, 0], 1).start()
            z_copy(p, b_, 0, ssem, rsem.at[u, 1], NZ - 1).start()
        elif s < 4:
            z_copy(p, b_, NZ - s, ssem, rsem.at[u, 2 * s - 2], 1).wait_recv()
            if s < 3:
                z_copy(p, b_, NZ - s, ssem, rsem.at[u, 2 * s], 1).start()
            elif not odd:
                z_copy(p, b_, 5, ssem, rsem.at[u, 6], 1).start()
            z_copy(p, b_, s, ssem, rsem.at[u, 2 * s - 1], NZ - 1).wait_recv()
            if s < 3:
                z_copy(p, b_, s, ssem, rsem.at[u, 2 * s + 1], NZ - 1).start()
            elif odd:
                z_copy(p, b_, 3, ssem, rsem.at[u, 6], NZ - 1).start()
        else:
            z_copy(p, b_, 4, ssem, rsem.at[u, 6], 1).wait_recv()

    def step(p, s):
        z_step(p, s, p, b, zsend, zrecv)
        if s == 0:
            b_both(p, 0)
        elif s < 4:
            b_both(p, 2 * s - 1)
            b_both(p, 2 * s)
        else:
            b_both(p, 7)

    def e_step(u, s):
        z_step(LAST, s, u, b_at((0, 1, 3, 2)[u]), ezsend, ezrecv)

    def e_along(_, s):
        if s == 0:
            e_copy(0, 0, 1).wait_recv()
            e_copy(1, 0, NB - 1).wait_recv()
            e_copy(2, NB - 1, 1).start()
        else:
            e_copy(2, NB - 1, 1).wait_recv()

    def forward(p, s):
        for j in ((0,), (1, 2), (3, 4), (5, 6), (7,))[s]:
            b_copy(p, j, j % 2).wait_recv()
            f_copy(p, j).start()

    def product(h, cols, wide, some):
        rows = jnp.concatenate(
            [some(z_at(dist(4 * h + k, k % 2))).reshape(NB * 16, wide) for k in range(4)], axis=0
        )
        for w in range(2):
            acc[h, w] += lax.dot_general(
                wbuf[w, :, cols], rows, (((1,), (1,)), ((), ())), preferred_element_type=F32
            )

    def multiply(p, h):
        for k in range(4):
            b_copy(p, 4 * h + k, 1 - k % 2, k % 2).wait_recv()
            f_copy(p, 4 * h + k, k % 2).wait_recv()
        cols = pl.ds(pl.multiple_of(p * WIDE, WIDE), WIDE)
        product(h, cols, WIDE, lambda zi: gath[p, zi])

    def multiply_last(h):
        product(h, columns(LAST), width - PIECES * WIDE, lambda zi: egath[zi])

    tile_rows(LAST)
    e_copy(0, 0, 1).start()
    e_copy(1, 0, NB - 1).start()
    for p in range(PIECES):
        tile_rows(p)
        step(p, 0)

    row = lax.broadcasted_iota(jnp.int32, (8, 128), 0)
    lane = lax.broadcasted_iota(jnp.int32, (8, 128), 1)
    base = b * 16 + a * 4

    def own_info():
        own = jnp.zeros((8, 128), jnp.int32)
        whole_last = (x == NA - 1) & (c == 1) & (z == NZ - 1) & (y == NB - 1)
        for t in range(4):
            seg = seg_s[t]
            if t < 3:
                kept = (pad_s[t] == 1) & (seg == seg_s[t + 1])
            else:
                kept = (pad_s[t] == 1) & jnp.logical_not(whole_last)
            code = jnp.where(kept, ben_s[seg], NBENCH)
            own = jnp.where(lane == base + t, tgt_s[t], own)
            own = jnp.where(lane == base + t + 64, code, own)
        return own.astype(F32)

    def along_info(_, s):
        if s == 0:
            wait_all(smalls)
            info[a * NB + b] = own_info()[0:1]
            start_all(planes(info, isend, irecv))
        elif s == 1:
            wait_all(planes(info, isend, irecv))
            info[NA * NB + z] = added(info, 0, NA * NB)
            start_all(lines(info, isend, irecv))
            start_all(crossings(info, xinfo, xisend, xirecv))
        else:
            wait_all(lines(info, isend, irecv))
            wait_all(crossings(info, xinfo, xisend, xirecv))

    index = ((x * 2 + c) * NZ + z) * NB + y
    other = ((x * 2 + 1 - c) * NZ + z) * NB + y
    entries = lax.broadcasted_iota(jnp.int32, (voc, 128), 0)
    numbers = [(entries + i * voc).astype(F32) for i in (index, other)]
    left = lane[0:1, :] < 64

    def over(line):
        return pltpu.roll(jnp.broadcast_to(line, (8, 128)), 64, 1)[0:1, :]

    def statistics(h):
        for k in (2 * h, 2 * h + 1):
            near = [z_at(dist(2 * k + m)) for m in range(2)]
            ends = [pl.ds(zi, 1) for zi in near]
            logits = [acc[k // 2, w, :, (k % 2) * 128 : (k % 2 + 1) * 128] for w in range(2)]
            wanted = jnp.where(left, info[NA * NB + near[0]], over(info[NA * NB + near[1]]))
            tops = [jnp.max(part, axis=0, keepdims=True) for part in logits]
            top = jnp.maximum(*tops)
            total = sum(jnp.sum(jnp.exp(part - top), axis=0, keepdims=True) for part in logits)
            picked = sum(
                jnp.sum(jnp.where(number == wanted, part, 0.0), axis=0, keepdims=True)
                for number, part in zip(numbers, logits)
            )
            lse = top + jnp.log(total)
            nllbuf[ends[0], :] = jnp.where(left, lse, over(picked))
            nllbuf[ends[1], :] = jnp.where(left, over(lse), picked)

    handle = {"lv": step, "fw": forward, "ez": e_step, "ef": e_along, "in": along_info}

    def slot(i):
        for k, things in enumerate(PLAN):

            @pl.when(i == k)
            def _():
                for what, which, s in things:
                    handle[what](which, s)
                if k < PIECES + 1:
                    own_weights(k).wait()
                    swap_weights(k).wait_recv()
                if k == 6:
                    statistics(0)

        p, h = lax.rem(i, PIECES + 1), i // (PIECES + 1)

        @pl.when(p < LAST)
        def _():
            multiply(p, h)

        @pl.when(p == LAST)
        def _():
            multiply_last(h)

    loop(len(PLAN), slot)
    statistics(1)
    def merged(buf, at, n):
        parts = [buf[at + k] for k in range(n)]
        top = functools.reduce(jnp.maximum, parts)
        total = functools.reduce(jnp.add, [jnp.exp(part - top) for part in parts])
        picked = functools.reduce(jnp.add, parts)
        return jnp.where(lane < 64, top + jnp.log(total), picked)

    stat[a * NB + b] = nllbuf[...]
    start_all(planes(stat, ssend, srecv))
    wait_all(planes(stat, ssend, srecv))
    stat[NA * NB + z] = merged(stat, 0, NA * NB)
    start_all(lines(stat, ssend, srecv))
    start_all(crossings(stat, xstat, xssend, xsrecv))
    def left_all(ref, ssem, rsem):
        rdma(ref, ref, ssem, rsem, partner).wait_send()

    left_all(abuf.at[:, 0:3], asend, arecv.at[0, 0])
    left_all(ebuf.at[0:3], easend, arecv.at[0, 0])
    rdma(weights, wbuf.at[1], wsend, wrecv.at[0], partner).wait_send()
    left_all(gath.at[:, 0:7, 0], zsend, zrecv.at[0, 0])
    left_all(gath.at[:, 0:4], bsend, brecv.at[0, 0, 0])
    left_all(gath.at[:, 0:2], fsend, frecv.at[0, 0])
    left_all(egath.at[0, 0:3], ebsend, ebrecv.at[0])
    left_all(egath.at[0:7], ezsend, ezrecv.at[0, 0])

    def losses(buf, at):
        both = merged(buf, at, NZ)
        return both - pltpu.roll(both, 64, 1)

    def gathered(buf, at):
        return jnp.concatenate([buf[at + k] for k in range(NZ)], axis=0)

    def by_core(mine, others, first, second):
        lower, upper = jnp.where(c == 0, mine, others), jnp.where(c == 0, others, mine)
        lower = pltpu.roll(lower, 64, 1) if first else lower
        upper = pltpu.roll(upper, 64, 1) if second else upper
        return jnp.where(lane < 64, lower, upper)

    codes = by_core(gathered(info, NA * NB), gathered(xinfo, 0), True, False)
    wait_all(lines(stat, ssend, srecv))
    nll = losses(stat, NA * NB)
    nllbuf[...] = nll
    mine = nllbuf[pl.ds(z, 1), :]
    rolled = pltpu.roll(jnp.broadcast_to(mine, (8, 128)), lax.rem(128 - base, 128), 1)
    wait_all(crossings(stat, xstat, xssend, xsrecv))
    loss = by_core(nll, losses(xstat, 0), False, True)
    last_t, last_c = jnp.zeros((8, 128), F32), jnp.zeros((8, 128), F32)
    for j in range(NBENCH):
        hit = codes == float(j)
        part_t = jnp.sum(jnp.where(hit, loss, 0.0), axis=0, keepdims=True)
        part_c = jnp.sum(jnp.where(hit, 1.0, 0.0), axis=0, keepdims=True)
        last_t = jnp.where(row == j, part_t, last_t)
        last_c = jnp.where(row == j, part_c, last_c)
    sums = jnp.sum(jnp.concatenate([last_t, last_c], axis=0), axis=1, keepdims=True)
    row16 = lax.broadcasted_iota(jnp.int32, (16, 128), 0)
    lane16 = lax.broadcasted_iota(jnp.int32, (16, 128), 1)
    sums = jnp.sum(jnp.where(lane16 == row16 + 4, sums, 0.0), axis=0, keepdims=True)
    out[...] = jnp.where(lane[0:1, :] < 4, rolled[0:1, :], sums)


def body(hidden, lm_head, targets, segment, pad_mask, seq_bench):
    tok, width = hidden.shape
    voc = lm_head.shape[1]
    rest = width - PIECES * WIDE
    tokens = GROUP * tok
    dma = pltpu.SemaphoreType.DMA
    anywhere = pl.BlockSpec(memory_space=pl.ANY)
    vmem = pl.BlockSpec(memory_space=pltpu.VMEM)
    out = pl.pallas_call(
        kernel,
        out_shape=jax.ShapeDtypeStruct((1, 128), F32),
        in_specs=[anywhere] * 6,
        out_specs=vmem,
        scratch_shapes=[
            pltpu.SMEM((tok,), jnp.int32),
            pltpu.SMEM((tok,), jnp.int32),
            pltpu.SMEM((tok,), jnp.int32),
            pltpu.SMEM(seq_bench.shape, jnp.int32),
            pltpu.VMEM((PIECES, NA, tok, WIDE), jnp.bfloat16),
            pltpu.VMEM((NA, tok, rest), jnp.bfloat16),
            pltpu.VMEM((NA * tok, WIDE), F32),
            pltpu.VMEM((PIECES, NZ, NB, NA * tok, WIDE), jnp.bfloat16),
            pltpu.VMEM((NZ, NB, NA * tok, rest), jnp.bfloat16),
            pltpu.VMEM((2, voc, width), jnp.bfloat16),
            pltpu.VMEM((2, 2, voc, tokens // 2), F32),
            pltpu.VMEM((NA * NB + NZ, 1, 128), F32),
            pltpu.VMEM((NA * NB + NZ, 8, 128), F32),
            pltpu.VMEM((NZ, 1, 128), F32),
            pltpu.VMEM((NZ, 8, 128), F32),
            pltpu.VMEM((8, 128), F32),
            dma((4,)), dma((PIECES + 1,)), dma((PIECES + 1,)), dma, dma((PIECES + 1,)),
            dma, dma, dma((PIECES + 1, NA - 1)), dma, dma((PIECES, NZ - 1)),
            dma, dma((PIECES, 2, NZ)), dma, dma((PIECES, NZ)),
            dma, dma((3,)), dma, dma((NB, NZ - 1)),
            dma((NA * NB + NZ,)), dma((NA * NB + NZ,)),
            dma((NA * NB + NZ,)), dma((NA * NB + NZ,)),
            dma((NZ,)), dma((NZ,)), dma((NZ,)), dma((NZ,)),
        ],
        compiler_params=pltpu.CompilerParams(
            collective_id=0, has_side_effects=True, vmem_limit_bytes=62 * 1024 * 1024
        ),
        name="nll",
    )(hidden, lm_head.T, targets, segment, pad_mask, seq_bench)

    def split(line, first, second, third):
        first[...] = line[:, 0:tok]
        second[...] = line[:, tok : tok + NBENCH]
        third[...] = line[:, tok + NBENCH : tok + 2 * NBENCH]

    nll, total, count = pl.pallas_call(
        split,
        out_shape=(
            jax.ShapeDtypeStruct((1, tok), F32),
            jax.ShapeDtypeStruct((1, NBENCH), F32),
            jax.ShapeDtypeStruct((1, NBENCH), F32),
        ),
        name="split",
    )(out)
    return (nll.reshape(tok), total.reshape(NBENCH), count.reshape(NBENCH))


def solution(mesh):
    split = Mesh(mesh.devices.reshape(4, 2, 8, 4), AXES)
    return jax.shard_map(
        body,
        mesh=split,
        in_specs=(P(AXES, None), P(None, AXES), P(AXES), P(AXES), P(AXES), P()),
        out_specs=(P(AXES), P(), P()),
        check_vma=False,
    )
```

```python
import functools

import jax
import jax.numpy as jnp
from jax import lax
from jax.experimental import pallas as pl
from jax.experimental.pallas import tpu as pltpu
from jax.sharding import Mesh
from jax.sharding import PartitionSpec as P

NBENCH = 8
AXES = ("dp_0", "dp_1", "vocab_0", "vocab_1")
NA, NB, NZ = 4, 4, 8
PIECES = 3
WIDE = 2304
LAST = PIECES
GROUP = NA * NB * NZ
PLAN = (
    (
        ("ef", 0, 0), ("fw", 0, 0), ("lv", 0, 1), ("lv", 1, 1), ("lv", 2, 1), ("lv", 0, 2),
        ("fw", 1, 0), ("lv", 1, 2), ("ef", 0, 1), ("in", 0, 0), ("ez", 3, 0), ("lv", 2, 2),
        ("fw", 2, 1), ("fw", 0, 1), ("fw", 0, 2), ("ez", 2, 0), ("fw", 1, 1), ("lv", 0, 3),
        ("ez", 1, 0), ("ez", 0, 0), ("fw", 2, 0), ("ez", 3, 1), ("fw", 1, 2), ("fw", 2, 2),
        ("ez", 2, 1), ("lv", 1, 3), ("lv", 0, 4), ("in", 0, 1), ("lv", 2, 3),
    ),
    (("ez", 1, 1), ("ez", 0, 1)),
    (("ez", 3, 2), ("fw", 0, 3), ("ez", 2, 2), ("lv", 1, 4)),
    (
        ("lv", 2, 4), ("fw", 0, 4), ("ez", 1, 2), ("fw", 1, 3), ("ez", 0, 2), ("fw", 1, 4),
    ),
    (("fw", 2, 3), ("ez", 2, 3), ("fw", 2, 4), ("ez", 3, 3)),
    (("ez", 1, 3), ("ez", 0, 3), ("in", 0, 2)),
    (("ez", 3, 4), ("ez", 2, 4)),
    (("ez", 1, 4), ("ez", 0, 4)),
)
FAR_PLANE = (10, 2, 8, 6, 9, 11, 14, 1, 3, 4, 12, 5, 7, 13, 15)
FAR_LINE = (4, 3, 5, 2, 6, 1, 7)
MESH = pl.DeviceIdType.MESH
F32 = jnp.float32


def kernel(
    hidden, weights, targets, segment, pad_mask, seq_bench,
    out,
    tgt_s, seg_s, pad_s, ben_s,
    abuf, ebuf, rows32, gath, egath, wbuf, acc, info, stat, xinfo, xstat, nllbuf,
    small, lsem, wlsem, wsend, wrecv, asend, easend, arecv, zsend, zrecv,
    bsend, brecv, fsend, frecv, ebsend, ebrecv, ezsend, ezrecv,
    isend, irecv, ssend, srecv, xisend, xirecv, xssend, xsrecv,
):
    x, c = lax.axis_index("dp_0"), lax.axis_index("dp_1")
    z, y = lax.axis_index("vocab_0"), lax.axis_index("vocab_1")
    a = y * (1 - c) + x * c
    b = x * (1 - c) + y * c
    width = weights.shape[1]
    voc = weights.shape[0]

    def dev(a_, b_, z_):
        return (b_ * (1 - c) + a_ * c, c, z_, a_ * (1 - c) + b_ * c)

    def rdma(src, dst, ssem, rsem, to):
        return pltpu.make_async_remote_copy(
            src_ref=src, dst_ref=dst, send_sem=ssem, recv_sem=rsem,
            device_id=to, device_id_type=MESH,
        )

    def a_at(k):
        return lax.rem(a + k, NA)

    def b_at(k):
        return lax.rem(b + k, NB)

    def z_at(k):
        return lax.rem(z + k, NZ)

    partner = (x, 1 - c, z, y)

    def columns(p):
        return slice(p * WIDE, (p + 1) * WIDE if p < LAST else width)

    def held(p):
        return abuf.at[p] if p < LAST else ebuf

    def own_hidden(p):
        return pltpu.make_async_copy(hidden.at[:, columns(p)], held(p).at[a], lsem.at[p])

    def own_weights(p):
        cols = columns(p)
        return pltpu.make_async_copy(weights.at[:, cols], wbuf.at[0, :, cols], wlsem.at[p])

    def swap_weights(p):
        cols = columns(p)
        return rdma(weights.at[:, cols], wbuf.at[1, :, cols], wsend, wrecv.at[p], partner)

    def loop(n, fn):
        lax.fori_loop(0, n, lambda i, _: (fn(i), 0)[1], 0)

    turns = (LAST, *range(PIECES))
    for p in turns:
        own_hidden(p).start()
    smalls = [
        pltpu.make_async_copy(src, dst, small.at[k])
        for k, (src, dst) in enumerate(
            ((targets, tgt_s), (segment, seg_s), (pad_mask, pad_s), (seq_bench, ben_s))
        )
    ]
    for copy in smalls:
        copy.start()

    barrier = pltpu.get_barrier_semaphore()
    peers = [dev(a_at(k), b, z) for k in range(1, NA)]
    peers += [dev(a, b_at(k), z) for k in (1, NB - 1)]
    peers += [dev(a, b, z_at(k)) for k in (1, NZ - 1)]
    peers += [partner]
    for peer in peers:
        pl.semaphore_signal(barrier, inc=1, device_id=peer, device_id_type=MESH)
    pl.semaphore_wait(barrier, len(peers))

    def a_copy(p, k):
        ssem = asend if p < LAST else easend
        mine = held(p).at[a]
        return rdma(mine, mine, ssem, arecv.at[p, k - 1], dev(a_at(k), b, z))

    for p in turns:
        own_hidden(p).wait()
        for k in range(1, NA):
            a_copy(p, k).start()
    for p in range(PIECES + 1):
        own_weights(p).start()
    for p in range(PIECES + 1):
        swap_weights(p).start()
    acc[...] = jnp.zeros(acc.shape, F32)

    def planes(buf, ssem, rsem):
        at = a * NB + b
        return [
            rdma(buf.at[at], buf.at[at], ssem.at[k], rsem.at[k], dev(a_at(k // NB), b_at(k % NB), z))
            for k in FAR_PLANE
        ]

    def lines(buf, ssem, rsem):
        at = NA * NB + z
        return [
            rdma(
                buf.at[at], buf.at[at], ssem.at[NA * NB + k], rsem.at[NA * NB + k],
                dev(a, b, z_at(k)),
            )
            for k in FAR_LINE
        ]

    def crossings(buf, far, ssem, rsem):
        return [
            rdma(
                buf.at[NA * NB + z], far.at[z], ssem.at[k], rsem.at[k], (x, 1 - c, z_at(k), y)
            )
            for k in (*FAR_LINE, 0)
        ]

    def start_all(copies):
        for copy in copies:
            copy.start()

    def wait_all(copies):
        for copy in copies:
            copy.wait()

    def added(buf, at, n):
        total = buf[at]
        for k in range(1, n):
            total = total + buf[at + k]
        return total

    def dist(j, odd=None):
        odd = j % 2 if odd is None else odd
        return NZ - 1 - j // 2 if odd else j // 2

    def block(p, b_, z_):
        return egath.at[z_, b_] if p is LAST else gath.at[p, z_, b_]

    def z_copy(p, b_, k, ssem, rsem, up):
        mine = block(p, b_, z_at(k))
        return rdma(mine, mine, ssem, rsem, dev(a, b, z_at(up)))

    def b_send(p, zi, b_, ssem, rsem, go):
        mine = block(p, b_, zi)
        return rdma(mine, mine, ssem, rsem, dev(a, b_at(go), z))

    def b_copy(p, j, way, odd=None):
        go = 1 if way == 0 else NB - 1
        return b_send(p, z_at(dist(j, odd)), b, bsend, brecv.at[p, way, j], go)

    def f_copy(p, j, odd=None):
        odd = j % 2 if odd is None else odd
        come, go = (1, NB - 1) if odd else (NB - 1, 1)
        return b_send(p, z_at(dist(j, odd)), b_at(come), fsend, frecv.at[p, j], go)

    def b_both(p, j):
        b_copy(p, j, 0).start()
        b_copy(p, j, 1).start()

    def e_copy(k, src, go):
        return b_send(LAST, z, b_at(src), ebsend, ebrecv.at[k], go)

    def tile_rows(p):
        wide = held(p).shape[2]
        for k in range(1, NA):
            a_copy(p, k).wait_recv()
        for k in range(NA):
            rows32[4 * k : 4 * k + 4, 0:wide] = held(p)[k].astype(F32)
        tile = rows32[:, 0:wide].astype(jnp.bfloat16)
        if p < LAST:
            gath[p, z, b] = tile
        else:
            egath[z, b] = tile

    def z_step(p, s, u, b_, ssem, rsem):
        odd = u % 2
        if s == 0:
            z_copy(p, b_, 0, ssem, rsem.at[u, 0], 1).start()
            z_copy(p, b_, 0, ssem, rsem.at[u, 1], NZ - 1).start()
        elif s < 4:
            z_copy(p, b_, NZ - s, ssem, rsem.at[u, 2 * s - 2], 1).wait_recv()
            if s < 3:
                z_copy(p, b_, NZ - s, ssem, rsem.at[u, 2 * s], 1).start()
            elif not odd:
                z_copy(p, b_, 5, ssem, rsem.at[u, 6], 1).start()
            z_copy(p, b_, s, ssem, rsem.at[u, 2 * s - 1], NZ - 1).wait_recv()
            if s < 3:
                z_copy(p, b_, s, ssem, rsem.at[u, 2 * s + 1], NZ - 1).start()
            elif odd:
                z_copy(p, b_, 3, ssem, rsem.at[u, 6], NZ - 1).start()
        else:
            z_copy(p, b_, 4, ssem, rsem.at[u, 6], 1).wait_recv()

    def step(p, s):
        z_step(p, s, p, b, zsend, zrecv)
        if s == 0:
            b_both(p, 0)
        elif s < 4:
            b_both(p, 2 * s - 1)
            b_both(p, 2 * s)
        else:
            b_both(p, 7)

    def e_step(u, s):
        z_step(LAST, s, u, b_at((0, 1, 3, 2)[u]), ezsend, ezrecv)

    def e_along(_, s):
        if s == 0:
            e_copy(0, 0, 1).wait_recv()
            e_copy(1, 0, NB - 1).wait_recv()
            e_copy(2, NB - 1, 1).start()
        else:
            e_copy(2, NB - 1, 1).wait_recv()

    def forward(p, s):
        for j in ((0,), (1, 2), (3, 4), (5, 6), (7,))[s]:
            b_copy(p, j, j % 2).wait_recv()
            f_copy(p, j).start()

    def product(h, cols, wide, some):
        rows = jnp.concatenate(
            [some(z_at(dist(4 * h + k, k % 2))).reshape(NB * 16, wide) for k in range(4)], axis=0
        )
        for w in range(2):
            acc[h, w] += lax.dot_general(
                wbuf[w, :, cols], rows, (((1,), (1,)), ((), ())), preferred_element_type=F32
            )

    def multiply(p, h):
        for k in range(4):
            b_copy(p, 4 * h + k, 1 - k % 2, k % 2).wait_recv()
            f_copy(p, 4 * h + k, k % 2).wait_recv()
        cols = pl.ds(pl.multiple_of(p * WIDE, WIDE), WIDE)
        product(h, cols, WIDE, lambda zi: gath[p, zi])

    def multiply_last(h):
        product(h, columns(LAST), width - PIECES * WIDE, lambda zi: egath[zi])

    tile_rows(LAST)
    e_copy(0, 0, 1).start()
    e_copy(1, 0, NB - 1).start()
    for p in range(PIECES):
        tile_rows(p)
        step(p, 0)

    row = lax.broadcasted_iota(jnp.int32, (8, 128), 0)
    lane = lax.broadcasted_iota(jnp.int32, (8, 128), 1)
    base = b * 16 + a * 4

    def own_info():
        own = jnp.zeros((8, 128), jnp.int32)
        whole_last = (x == NA - 1) & (c == 1) & (z == NZ - 1) & (y == NB - 1)
        for t in range(4):
            seg = seg_s[t]
            if t < 3:
                kept = (pad_s[t] == 1) & (seg == seg_s[t + 1])
            else:
                kept = (pad_s[t] == 1) & jnp.logical_not(whole_last)
            code = jnp.where(kept, ben_s[seg], NBENCH)
            own = jnp.where(lane == base + t, tgt_s[t], own)
            own = jnp.where(lane == base + t + 64, code, own)
        return own.astype(F32)

    def along_info(_, s):
        if s == 0:
            wait_all(smalls)
            info[a * NB + b] = own_info()[0:1]
            start_all(planes(info, isend, irecv))
        elif s == 1:
            wait_all(planes(info, isend, irecv))
            info[NA * NB + z] = added(info, 0, NA * NB)
            start_all(lines(info, isend, irecv))
            start_all(crossings(info, xinfo, xisend, xirecv))
        else:
            wait_all(lines(info, isend, irecv))
            wait_all(crossings(info, xinfo, xisend, xirecv))

    index = ((x * 2 + c) * NZ + z) * NB + y
    other = ((x * 2 + 1 - c) * NZ + z) * NB + y
    entries = lax.broadcasted_iota(jnp.int32, (voc, 128), 0)
    numbers = [(entries + i * voc).astype(F32) for i in (index, other)]
    left = lane[0:1, :] < 64

    def over(line):
        return pltpu.roll(jnp.broadcast_to(line, (8, 128)), 64, 1)[0:1, :]

    def statistics(h):
        for k in (2 * h, 2 * h + 1):
            near = [z_at(dist(2 * k + m)) for m in range(2)]
            ends = [pl.ds(zi, 1) for zi in near]
            logits = [acc[k // 2, w, :, (k % 2) * 128 : (k % 2 + 1) * 128] for w in range(2)]
            wanted = jnp.where(left, info[NA * NB + near[0]], over(info[NA * NB + near[1]]))
            tops = [jnp.max(part, axis=0, keepdims=True) for part in logits]
            top = jnp.maximum(*tops)
            total = sum(jnp.sum(jnp.exp(part - top), axis=0, keepdims=True) for part in logits)
            picked = sum(
                jnp.sum(jnp.where(number == wanted, part, 0.0), axis=0, keepdims=True)
                for number, part in zip(numbers, logits)
            )
            lse = top + jnp.log(total)
            nllbuf[ends[0], :] = jnp.where(left, lse, over(picked))
            nllbuf[ends[1], :] = jnp.where(left, over(lse), picked)

    handle = {"lv": step, "fw": forward, "ez": e_step, "ef": e_along, "in": along_info}

    def slot(i):
        for k, things in enumerate(PLAN):

            @pl.when(i == k)
            def _():
                for what, which, s in things:
                    handle[what](which, s)
                if k < PIECES + 1:
                    own_weights(k).wait()
                    swap_weights(k).wait_recv()
                if k == 6:
                    statistics(0)

        p, h = lax.rem(i, PIECES + 1), i // (PIECES + 1)

        @pl.when(p < LAST)
        def _():
            multiply(p, h)

        @pl.when(p == LAST)
        def _():
            multiply_last(h)

    loop(len(PLAN), slot)
    statistics(1)
    def merged(buf, at, n):
        parts = [buf[at + k] for k in range(n)]
        top = functools.reduce(jnp.maximum, parts)
        total = functools.reduce(jnp.add, [jnp.exp(part - top) for part in parts])
        picked = functools.reduce(jnp.add, parts)
        return jnp.where(lane < 64, top + jnp.log(total), picked)

    stat[a * NB + b] = nllbuf[...]
    start_all(planes(stat, ssend, srecv))
    wait_all(planes(stat, ssend, srecv))
    stat[NA * NB + z] = merged(stat, 0, NA * NB)
    start_all(crossings(stat, xstat, xssend, xsrecv))
    start_all(lines(stat, ssend, srecv))
    def left_all(ref, ssem, rsem):
        rdma(ref, ref, ssem, rsem, partner).wait_send()

    left_all(abuf.at[:, 0:3], asend, arecv.at[0, 0])
    left_all(ebuf.at[0:3], easend, arecv.at[0, 0])
    rdma(weights, wbuf.at[1], wsend, wrecv.at[0], partner).wait_send()
    left_all(gath.at[:, 0:7, 0], zsend, zrecv.at[0, 0])
    left_all(gath.at[:, 0:4], bsend, brecv.at[0, 0, 0])
    left_all(gath.at[:, 0:2], fsend, frecv.at[0, 0])
    left_all(egath.at[0, 0:3], ebsend, ebrecv.at[0])
    left_all(egath.at[0:7], ezsend, ezrecv.at[0, 0])

    def losses(buf, at):
        both = merged(buf, at, NZ)
        return both - pltpu.roll(both, 64, 1)

    def gathered(buf, at):
        return jnp.concatenate([buf[at + k] for k in range(NZ)], axis=0)

    def by_core(mine, others, first, second):
        lower, upper = jnp.where(c == 0, mine, others), jnp.where(c == 0, others, mine)
        lower = pltpu.roll(lower, 64, 1) if first else lower
        upper = pltpu.roll(upper, 64, 1) if second else upper
        return jnp.where(lane < 64, lower, upper)

    codes = by_core(gathered(info, NA * NB), gathered(xinfo, 0), True, False)
    wait_all(lines(stat, ssend, srecv))
    nll = losses(stat, NA * NB)
    nllbuf[...] = nll
    mine = nllbuf[pl.ds(z, 1), :]
    rolled = pltpu.roll(jnp.broadcast_to(mine, (8, 128)), lax.rem(128 - base, 128), 1)
    wait_all(crossings(stat, xstat, xssend, xsrecv))
    loss = by_core(nll, losses(xstat, 0), False, True)
    last_t, last_c = jnp.zeros((8, 128), F32), jnp.zeros((8, 128), F32)
    for j in range(NBENCH):
        hit = codes == float(j)
        part_t = jnp.sum(jnp.where(hit, loss, 0.0), axis=0, keepdims=True)
        part_c = jnp.sum(jnp.where(hit, 1.0, 0.0), axis=0, keepdims=True)
        last_t = jnp.where(row == j, part_t, last_t)
        last_c = jnp.where(row == j, part_c, last_c)
    sums = jnp.sum(jnp.concatenate([last_t, last_c], axis=0), axis=1, keepdims=True)
    row16 = lax.broadcasted_iota(jnp.int32, (16, 128), 0)
    lane16 = lax.broadcasted_iota(jnp.int32, (16, 128), 1)
    sums = jnp.sum(jnp.where(lane16 == row16 + 4, sums, 0.0), axis=0, keepdims=True)
    out[...] = jnp.where(lane[0:1, :] < 4, rolled[0:1, :], sums)


def body(hidden, lm_head, targets, segment, pad_mask, seq_bench):
    tok, width = hidden.shape
    voc = lm_head.shape[1]
    rest = width - PIECES * WIDE
    tokens = GROUP * tok
    dma = pltpu.SemaphoreType.DMA
    anywhere = pl.BlockSpec(memory_space=pl.ANY)
    vmem = pl.BlockSpec(memory_space=pltpu.VMEM)
    out = pl.pallas_call(
        kernel,
        out_shape=jax.ShapeDtypeStruct((1, 128), F32),
        in_specs=[anywhere] * 6,
        out_specs=vmem,
        scratch_shapes=[
            pltpu.SMEM((tok,), jnp.int32),
            pltpu.SMEM((tok,), jnp.int32),
            pltpu.SMEM((tok,), jnp.int32),
            pltpu.SMEM(seq_bench.shape, jnp.int32),
            pltpu.VMEM((PIECES, NA, tok, WIDE), jnp.bfloat16),
            pltpu.VMEM((NA, tok, rest), jnp.bfloat16),
            pltpu.VMEM((NA * tok, WIDE), F32),
            pltpu.VMEM((PIECES, NZ, NB, NA * tok, WIDE), jnp.bfloat16),
            pltpu.VMEM((NZ, NB, NA * tok, rest), jnp.bfloat16),
            pltpu.VMEM((2, voc, width), jnp.bfloat16),
            pltpu.VMEM((2, 2, voc, tokens // 2), F32),
            pltpu.VMEM((NA * NB + NZ, 1, 128), F32),
            pltpu.VMEM((NA * NB + NZ, 8, 128), F32),
            pltpu.VMEM((NZ, 1, 128), F32),
            pltpu.VMEM((NZ, 8, 128), F32),
            pltpu.VMEM((8, 128), F32),
            dma((4,)), dma((PIECES + 1,)), dma((PIECES + 1,)), dma, dma((PIECES + 1,)),
            dma, dma, dma((PIECES + 1, NA - 1)), dma, dma((PIECES, NZ - 1)),
            dma, dma((PIECES, 2, NZ)), dma, dma((PIECES, NZ)),
            dma, dma((3,)), dma, dma((NB, NZ - 1)),
            dma((NA * NB + NZ,)), dma((NA * NB + NZ,)),
            dma((NA * NB + NZ,)), dma((NA * NB + NZ,)),
            dma((NZ,)), dma((NZ,)), dma((NZ,)), dma((NZ,)),
        ],
        compiler_params=pltpu.CompilerParams(
            collective_id=0, has_side_effects=True, vmem_limit_bytes=62 * 1024 * 1024
        ),
        name="nll",
    )(hidden, lm_head.T, targets, segment, pad_mask, seq_bench)

    def split(line, first, second, third):
        first[...] = line[:, 0:tok]
        second[...] = line[:, tok : tok + NBENCH]
        third[...] = line[:, tok + NBENCH : tok + 2 * NBENCH]

    nll, total, count = pl.pallas_call(
        split,
        out_shape=(
            jax.ShapeDtypeStruct((1, tok), F32),
            jax.ShapeDtypeStruct((1, NBENCH), F32),
            jax.ShapeDtypeStruct((1, NBENCH), F32),
        ),
        name="split",
    )(out)
    return (nll.reshape(tok), total.reshape(NBENCH), count.reshape(NBENCH))


def solution(mesh):
    split = Mesh(mesh.devices.reshape(4, 2, 8, 4), AXES)
    return jax.shard_map(
        body,
        mesh=split,
        in_specs=(P(AXES, None), P(None, AXES), P(AXES), P(AXES), P(AXES), P()),
        out_specs=(P(AXES), P(), P()),
        check_vma=False,
    )
```
